32 devices in a mesh: role: 2 (over core), shard: 16 (over z, y, x).
Axes of the slice: x: 2, y: 2, z: 4, core: 2. Of those that a mesh axis runs over, the one named last changes fastest.
Arguments:
- history: bfloat16 [256, 640, 128], P(None, ('role', 'shard')), may hold values from -20 to 20
- event_cat: int32 [256, 640], P(None, ('role', 'shard')), may hold values from 0 to 1023, as said below
- candidates: bfloat16 [256, 200, 128], P(('role', 'shard')), may hold values from -9 to 9
- cand_cat: int32 [256, 200], P(('role', 'shard')), may hold values from 0 to 1023, as said below
- w_input: bfloat16 [256, 512], replicated, may hold values from -0.375 to 0.375
- w_output: bfloat16 [512, 128], replicated, may hold values from -0.25 to 0.25
Outputs:
- interest_features: bfloat16 [256, 200, 128], P(('role', 'shard'))
The draws below stay inside these ranges and needn't reach their ends.
Inputs may be any that keep to these rules, and one draw needn't show every extreme that they name: `event_cat`: in each aligned block of 20 events of one user, at most 8 events have a category that some candidate of that user has; users 2 i and 2 i + 1 have exactly 8 such events together in every block; every user has a block with exactly 8. `cand_cat`: the candidates of one user carry at most 8 distinct categories.
All inputs are finite; a program needn't handle non-finite values.
Results may differ from the reference program's by a relative error of at most 0.0095.
Values may be sent and summed in bfloat16 or wider, within the bound.
No kernel may reach another device: no remote copies, remote signals or barrier semaphores. Data moves between devices by JAX's collectives and lax.ppermute only.
A program may use at most 64 MiB of HBM per device.

```python
import math
import jax
import jax.numpy as jnp
from jax import lax

D = 128
HEADS = 4
HID = 512
NCAT = 1024
CANDS = 200
QCAT = 8
CAP = 8
E_DEV = 20
USERS = 256
EVENTS = 640


def user_base(key):
    return jax.random.randint(jax.random.fold_in(key, 101), (USERS,), 0, NCAT)


def draw_cand_cat(key, part):
    base = user_base(key)
    user_keys = jax.random.split(jax.random.fold_in(key, 111), USERS)
    orders = jax.vmap(lambda single: jax.random.permutation(single, CANDS))(user_keys)
    inverse = jnp.argsort(orders, axis=1).astype(jnp.int32)
    picked = jax.random.randint(jax.random.fold_in(key, 112), (USERS, CANDS), 0, QCAT)
    offset = jnp.where(inverse < QCAT, inverse, picked)
    return ((base[:, None] + offset) % NCAT).astype(jnp.int32)


def draw_event_cat(key, part):
    base = user_base(key)
    blocks = EVENTS // E_DEV
    pairs = USERS // 2
    first = jax.random.randint(jax.random.fold_in(key, 121), (pairs, blocks), 0, CAP + 1)
    full_block = jax.random.randint(jax.random.fold_in(key, 122), (pairs,), 0, blocks)
    empty_block = (full_block + 1 + jax.random.randint(jax.random.fold_in(key, 126), (pairs,), 0, blocks - 1)) % blocks
    block_ids = jnp.arange(blocks)[None, :]
    first = jnp.where(block_ids == full_block[:, None], CAP, first)
    first = jnp.where(block_ids == empty_block[:, None], 0, first)
    counts = jnp.stack([first, CAP - first], axis=1).reshape(USERS, blocks)
    block_keys = jax.random.split(jax.random.fold_in(key, 123), USERS * blocks)
    orders = jax.vmap(lambda single: jax.random.permutation(single, E_DEV))(block_keys).reshape(USERS, blocks, E_DEV)
    matched = orders < counts[:, :, None]
    inside = jax.random.randint(jax.random.fold_in(key, 124), (USERS, blocks, E_DEV), 0, QCAT)
    outside = jax.random.randint(jax.random.fold_in(key, 125), (USERS, blocks, E_DEV), QCAT, NCAT)
    offset = jnp.where(matched, inside, outside)
    return ((base[:, None, None] + offset) % NCAT).reshape(USERS, EVENTS).astype(jnp.int32)


def draw_history(key, part):
    noise_key = jax.random.fold_in(key, 303)

    def one_user(index):
        single = jax.random.fold_in(noise_key, index)
        noise = jnp.clip(jax.random.normal(single, (EVENTS, D), jnp.float32), -6.0, 6.0)
        return noise.astype(jnp.bfloat16)
    return lax.map(one_user, jnp.arange(USERS, dtype=jnp.int32))


def draw_candidates(key, part):
    values = jnp.clip(1.5 * jax.random.normal(jax.random.fold_in(key, 404), (USERS, CANDS, D), jnp.float32), -9.0, 9.0)
    return values.astype(jnp.bfloat16)


def scatter_about(own_key, extent, scale, reach, kind=jnp.bfloat16):
    entries = jax.random.normal(own_key, extent, jnp.float32) * scale
    return jnp.minimum(jnp.maximum(entries, -reach), reach).astype(kind)


def setup_inputs(seed: int = 0) -> dict:
    keys = jax.random.split(jax.random.key(seed), 7)
    return {
        "history": draw_history(jax.random.fold_in(keys[6], 71), 0),
        "event_cat": draw_event_cat(jax.random.fold_in(keys[6], 71), 0),
        "candidates": draw_candidates(jax.random.fold_in(keys[6], 71), 0),
        "cand_cat": draw_cand_cat(jax.random.fold_in(keys[6], 71), 0),
        "w_input": scatter_about(keys[4], (2 * D, HID), (2 * D) ** -0.5, 0.375),
        "w_output": scatter_about(keys[5], (HID, D), HID ** -0.5, 0.25),
    }


def attend(queries, slots, usable):
    group = queries.shape[0]
    count = queries.shape[1]
    width = queries.shape[2]
    head_size = width // HEADS
    query_heads = queries.astype(jnp.float32).reshape(group, count, HEADS, head_size)
    key_heads = slots.astype(jnp.float32).reshape(group, -1, HEADS, head_size)
    scores = jnp.einsum("gchk,gshk->ghcs", query_heads, key_heads) * (head_size ** -0.5)
    scores = jnp.where(usable[:, None, None, :], scores, -1e30)
    row_max = jnp.max(scores, axis=-1, keepdims=True)
    expo = jnp.exp(scores - row_max)
    total = jnp.sum(expo, axis=-1, keepdims=True)
    weights = (expo / total).astype(jnp.bfloat16)
    interest = jnp.einsum("ghcs,gshk->gchk", weights.astype(jnp.float32), key_heads)
    return interest.reshape(group, count, width).astype(jnp.bfloat16)


def user_group(history, event_cat, candidates, cand_cat, w_input, w_output):
    group = history.shape[0]
    blocks = EVENTS // E_DEV
    hits = jnp.any(event_cat[:, :, None] == cand_cat[:, None, :], axis=-1).reshape(group, blocks, E_DEV)
    slot_rank = jnp.cumsum(hits.astype(jnp.int32), axis=-1) - 1
    places = jnp.arange(CAP, dtype=jnp.int32)
    selector = (hits[:, :, None, :] & (slot_rank[:, :, None, :] == places[None, None, :, None])).astype(jnp.float32)
    events = history.reshape(group, blocks, E_DEV, D).astype(jnp.float32)
    slots = jnp.einsum("gbse,gbed->gbsd", selector, events).astype(jnp.bfloat16).reshape(group, blocks * CAP, D)
    counts = jnp.sum(hits.astype(jnp.int32), axis=-1)
    usable = (places[None, None, :] < counts[:, :, None]).reshape(group, blocks * CAP)
    interest = attend(candidates, slots, usable)
    rows = group * CANDS
    hidden = jnp.dot(candidates.reshape(rows, D), w_input[:D], preferred_element_type=jnp.float32)
    hidden = hidden + jnp.dot(interest.reshape(rows, D), w_input[D:], preferred_element_type=jnp.float32)
    hidden = jax.nn.silu(hidden).astype(jnp.bfloat16)
    result = jnp.dot(hidden, w_output, preferred_element_type=jnp.float32).astype(jnp.bfloat16)
    return result.reshape(group, CANDS, D)


def reference(history, event_cat, candidates, cand_cat, w_input, w_output):
    group = math.gcd(USERS, 16)
    packs = USERS // group

    def one_pack(pieces):
        return user_group(pieces[0], pieces[1], pieces[2], pieces[3], w_input, w_output)

    result = lax.map(one_pack, (history.reshape(packs, group, EVENTS, D), event_cat.reshape(packs, group, EVENTS), candidates.reshape(packs, group, CANDS, D), cand_cat.reshape(packs, group, CANDS)))
    return result.reshape(USERS, CANDS, D)
```

```python
import math

import jax
import jax.numpy as jnp
from jax import lax
from jax.sharding import PartitionSpec as P

HEADS = 4
CAP = 8
QCAT = 8


def distinct_categories(cand_cat):
    beyond = jnp.iinfo(jnp.int32).max
    current = jnp.min(cand_cat, axis=1)
    found = [current]
    for _ in range(QCAT - 1):
        following = jnp.min(jnp.where(cand_cat > current[:, None], cand_cat, beyond), axis=1)
        current = jnp.where(following == beyond, current, following)
        found.append(current)
    return jnp.stack(found, axis=1)


def attend(queries, event_keys, allowed):
    group = queries.shape[0]
    count = queries.shape[1]
    width = queries.shape[2]
    head_size = width // HEADS
    query_heads = queries.reshape(group, count, HEADS, head_size)
    key_heads = event_keys.reshape(group, -1, HEADS, head_size)
    scores = jnp.einsum(
        "gchk,gshk->ghcs", query_heads, key_heads, preferred_element_type=jnp.float32
    ) * head_size ** (-0.5)
    scores = jnp.where(allowed[:, None, None, :], scores, -1e30)
    row_max = jnp.max(scores, axis=-1, keepdims=True)
    expo = jnp.exp(scores - row_max)
    total = jnp.sum(expo, axis=-1, keepdims=True)
    weights = (expo / total).astype(jnp.bfloat16)
    interest = jnp.einsum("ghcs,gshk->gchk", weights, key_heads, preferred_element_type=jnp.float32)
    return interest.reshape(group, count, width).astype(jnp.bfloat16)


def local(history, event_cat, candidates, cand_cat, w_input, w_output):
    devices = lax.axis_size(("role", "shard"))
    own_wanted = distinct_categories(cand_cat).reshape(1, 1, -1)
    wanted = lax.all_to_all(
        jnp.broadcast_to(own_wanted, (devices, 1, own_wanted.shape[2])),
        ("role", "shard"),
        split_axis=0,
        concat_axis=0,
        tiled=True,
    ).reshape(-1, QCAT)
    hits = jnp.any(event_cat[:, :, None] == wanted[:, None, :], axis=-1)
    slot_rank = jnp.cumsum(hits.astype(jnp.int32), axis=1) - 1
    places = jnp.arange(CAP, dtype=jnp.int32)
    place_values = places.astype(jnp.float32)
    own_users = candidates.shape[0]
    cand_count = candidates.shape[1]
    width = candidates.shape[2]
    rows = own_users * cand_count
    cand_part = jnp.dot(
        candidates.reshape(rows, width), w_input[:width], preferred_element_type=jnp.float32
    )
    hit_counts = jnp.sum(hits.astype(jnp.int32), axis=1)
    pair_counts = hit_counts.reshape(-1, 2)
    start = jnp.stack([jnp.zeros_like(pair_counts[:, 0]), pair_counts[:, 0]], axis=1).reshape(-1)
    shifted = slot_rank + start[:, None]
    selector = (hits[:, None, :] & (shifted[:, None, :] == places[None, :, None])).astype(
        jnp.bfloat16
    )
    spread = jnp.einsum("use,ued->usd", selector, history, preferred_element_type=jnp.float32)
    packed = jnp.sum(spread.reshape(-1, 2, CAP, width), axis=1).astype(jnp.bfloat16)
    received, counts_in = (
        lax.all_to_all(packed, ("role", "shard"), split_axis=0, concat_axis=1, tiled=True),
        lax.all_to_all(
            pair_counts.astype(jnp.bfloat16),
            ("role", "shard"),
            split_axis=0,
            concat_axis=1,
            tiled=True,
        ),
    )
    half = own_users // 2
    counts_in = counts_in.astype(jnp.float32).reshape(half, -1, 2)
    lead = counts_in[:, :, 0][:, :, None]
    follow = counts_in[:, :, 1][:, :, None]
    lead_use = place_values[None, None, :] < lead
    follow_use = (place_values[None, None, :] >= lead) & (
        place_values[None, None, :] < lead + follow
    )
    usable = jnp.stack([lead_use, follow_use], axis=1).reshape(own_users, -1)
    received = jnp.repeat(received, 2, axis=0)
    group = math.gcd(own_users, 4)
    packs = own_users // group

    def one_pack(pieces):
        return attend(pieces[0], pieces[1], pieces[2])

    interest = lax.map(
        one_pack,
        (
            candidates.reshape(packs, group, cand_count, width),
            received.reshape(packs, group, -1, width),
            usable.reshape(packs, group, -1),
        ),
    )
    interest = interest.reshape(rows, width)
    hidden = cand_part + jnp.dot(interest, w_input[width:], preferred_element_type=jnp.float32)
    hidden = jax.nn.silu(hidden).astype(jnp.bfloat16)
    result = jnp.dot(hidden, w_output, preferred_element_type=jnp.float32).astype(jnp.bfloat16)
    return result.reshape(own_users, cand_count, width)


def solution(mesh):
    placed = (
        P(None, ("role", "shard"), None),
        P(None, ("role", "shard")),
        P(("role", "shard"), None, None),
        P(("role", "shard"), None),
        P(),
        P(),
    )
    return jax.shard_map(
        local,
        mesh=mesh,
        in_specs=placed,
        out_specs=P(("role", "shard"), None, None),
        check_vma=False,
    )
```

```python
import math

import jax
import jax.numpy as jnp
from jax import lax
from jax.experimental import pallas as pl
from jax.experimental.pallas import tpu as pltpu
from jax.sharding import PartitionSpec as P

HEADS = 4
CAP = 8
QCAT = 8
LANES = 128
FINE = 8
BARRED = -1e30
AXES = ("role", "shard")


def iota(shape, dimension):
    return lax.broadcasted_iota(jnp.int32, shape, dimension)


def distinct_kernel(cat_ref, out_ref):
    cats = cat_ref[...].astype(jnp.float32)
    users = cats.shape[0]
    half = LANES // 2
    user = iota((users, LANES), 0)
    lane = iota((users, LANES), 1)
    beyond = jnp.float32(1e9)
    low = jnp.min(cats, axis=1, keepdims=True)
    high = jnp.max(cats, axis=1, keepdims=True)
    row = jnp.zeros((users, LANES), jnp.float32)
    for step in range(QCAT // 2):
        for place, value in ((step, low), (QCAT - 1 - step, high)):
            row = jnp.where(lane % half == place * users + user, value, row)
        if step + 1 < QCAT // 2:
            above = jnp.min(jnp.where(cats > low, cats, beyond), axis=1, keepdims=True)
            below = jnp.max(jnp.where(cats < high, cats, -beyond), axis=1, keepdims=True)
            low = jnp.where(above == beyond, low, above)
            high = jnp.where(below == -beyond, high, below)
    whole = jnp.sum(row, axis=0, keepdims=True).astype(jnp.int32)
    fine = whole & (FINE - 1)
    packed = jnp.where(iota((1, LANES), 1) < half, whole - fine, fine)
    out_ref[...] = jnp.broadcast_to(packed.reshape(1, 1, LANES), out_ref.shape)


def pack_kernel(wanted_ref, event_ref, history_ref, out_ref, *, own_users):
    devices = wanted_ref.shape[0]
    blocks_events = history_ref.shape[0]
    width = history_ref.shape[2]
    depth = event_ref.shape[1]
    span = depth // blocks_events
    per_group = span // own_users
    pairs = own_users // 2
    half = LANES // 2
    pad = -(-depth // LANES) * LANES
    wanted = wanted_ref[:, 0, :].astype(jnp.float32).astype(jnp.bfloat16)
    line = iota((LANES, pad), 0) % half
    mate = iota((LANES, pad), 1) % own_users
    events = event_ref[...].astype(jnp.float32)
    match = None
    for j in range(QCAT):
        spread = jnp.where(line == j * own_users + mate, 1.0, 0.0).astype(jnp.bfloat16)
        category = jnp.dot(wanted, spread, preferred_element_type=jnp.float32)[:, :depth]
        same = jnp.where(category == events, 1.0, 0.0)
        match = same if match is None else jnp.maximum(match, same)
    position = iota((devices, depth), 1) % span
    mine = position // own_users == iota((devices, depth), 0) % per_group
    match = jnp.where(mine, match, 0.0)
    before = iota((depth, pad), 0)
    here = iota((depth, pad), 1)
    user_before = before % span
    user_here = here % span
    counted = (user_before == user_here) & (before <= here)
    counted = counted | ((user_here % 2 == 1) & (user_before == user_here - 1))
    counted = jnp.where(counted, 1.0, 0.0).astype(jnp.bfloat16)
    matched = match.astype(jnp.bfloat16)
    place = jnp.dot(matched, counted, preferred_element_type=jnp.float32)[:, :depth]
    pair_base = ((position % own_users) // 2 * CAP - 1).astype(jnp.float32)
    code = jnp.where(match > 0.0, place + pair_base, -1.0)
    lane = iota((depth, LANES), 1)
    leading = (lane < 2 * pairs) & (iota((depth, LANES), 0) % own_users == 2 * (lane % pairs))
    leading = jnp.where(leading, 1.0, 0.0).astype(jnp.bfloat16)
    lead = jnp.dot(matched, leading, preferred_element_type=jnp.float32)
    rows = pairs * CAP
    row = iota((rows, depth), 0).astype(jnp.float32)
    rank = iota((CAP, LANES), 0).astype(jnp.float32)
    first = iota((CAP, LANES), 1) < pairs
    for group in range(devices // per_group):
        stored = history_ref[:, group * span : (group + 1) * span, :].reshape(depth, width)
        picks = []
        for member in range(per_group):
            device = group * per_group + member
            picks.append(jnp.where(row == code[device : device + 1, :], 1.0, 0.0).astype(jnp.bfloat16))
        packed = jnp.dot(jnp.concatenate(picks, axis=0), stored, preferred_element_type=jnp.float32)
        packed = packed.astype(jnp.bfloat16)
        for member in range(per_group):
            device = group * per_group + member
            out_ref[device, :rows, :] = packed[member * rows : (member + 1) * rows, :]
            is_lead = rank < lead[device : device + 1, :]
            barred = jnp.where(is_lead == first, 0.0, BARRED)
            out_ref[device, rows:, :] = barred.astype(jnp.bfloat16)


def tower_kernel(key_ref, bar_ref, cand_ref, w_in_ref, w_out_ref, out_ref, *, pairs):
    pair = pl.program_id(0)
    rows, width = cand_ref.shape
    slots = key_ref.shape[0] * CAP
    head_size = width // HEADS
    scale = math.log2(math.e) * head_size ** (-0.5)
    cands = cand_ref[...]
    keys = key_ref[...].reshape(slots, width)
    lane_row = iota((rows, LANES), 1)
    second = jnp.where(iota((rows, LANES), 0) >= rows // 2, pairs, 0)
    chosen = jnp.where(lane_row == pair + second, 1.0, 0.0).astype(jnp.bfloat16)
    right = jnp.concatenate([keys, bar_ref[...].reshape(slots, LANES)], axis=1)
    values = jnp.concatenate([keys, jnp.ones((slots, width), jnp.bfloat16)], axis=1)
    head_of = iota((rows, width), 1) // head_size
    interest = jnp.zeros((rows, width), jnp.float32)
    total = jnp.zeros((rows, width), jnp.float32)
    for head in range(HEADS):
        queries = jnp.where(head_of == head, cands.astype(jnp.float32), 0.0).astype(jnp.bfloat16)
        left = jnp.concatenate([queries, chosen], axis=1)
        scores = lax.dot_general(left, right, (((1,), (1,)), ((), ())), preferred_element_type=jnp.float32)
        peak = jnp.max(scores, axis=1, keepdims=True)
        expo = jnp.exp2((scores - peak) * scale).astype(jnp.bfloat16)
        both = jnp.dot(expo, values, preferred_element_type=jnp.float32)
        interest = jnp.where(head_of == head, both[:, :width], interest)
        total = jnp.where(head_of == head, both[:, width:], total)
    interest = (interest / total).astype(jnp.bfloat16)
    hidden = jnp.dot(
        jnp.concatenate([cands, interest], axis=1), w_in_ref[...], preferred_element_type=jnp.float32
    )
    middle = hidden * 0.5
    hidden = (middle * jnp.tanh(middle) + middle).astype(jnp.bfloat16)
    result = jnp.dot(hidden, w_out_ref[...], preferred_element_type=jnp.float32)
    out_ref[...] = result.astype(jnp.bfloat16)


def exchange(parts):
    return lax.all_to_all(parts, AXES, split_axis=0, concat_axis=0, tiled=True)


def local(history, event_cat, candidates, cand_cat, w_input, w_output):
    devices = lax.axis_size(AXES)
    own_users, cand_count, width = candidates.shape
    users, block_events = event_cat.shape
    pairs = own_users // 2
    wanted = pl.pallas_call(
        distinct_kernel,
        out_shape=jax.ShapeDtypeStruct((devices, 1, LANES), jnp.int32),
        name="distinct",
    )(cand_cat)
    wanted = exchange(wanted)
    span = math.lcm(16, own_users)
    grouped = event_cat.T.reshape(block_events, users // span, span).transpose(1, 0, 2)
    grouped = jnp.repeat(grouped.reshape(users // span, block_events * span), span // own_users, axis=0)
    packed = pl.pallas_call(
        lambda *refs: pack_kernel(*refs, own_users=own_users),
        out_shape=jax.ShapeDtypeStruct((devices, (pairs + 1) * CAP, width), jnp.bfloat16),
        name="pack",
    )(wanted, grouped, history.transpose(1, 0, 2))
    received = exchange(packed)
    rows = own_users * cand_count
    result = pl.pallas_call(
        lambda *refs: tower_kernel(*refs, pairs=pairs),
        out_shape=jax.ShapeDtypeStruct((rows, width), jnp.bfloat16),
        grid=(pairs,),
        in_specs=[
            pl.BlockSpec((devices, CAP, width), lambda i: (0, i, 0)),
            pl.BlockSpec((devices, CAP, width), lambda i: (0, pairs, 0)),
            pl.BlockSpec((rows // pairs, width), lambda i: (i, 0)),
            pl.BlockSpec(w_input.shape, lambda i: (0, 0)),
            pl.BlockSpec(w_output.shape, lambda i: (0, 0)),
        ],
        out_specs=pl.BlockSpec((rows // pairs, width), lambda i: (i, 0)),
        name="tower",
    )(received, received, candidates.reshape(rows, width), w_input, w_output)
    return result.reshape(own_users, cand_count, width)


def solution(mesh):
    placed = (
        P(None, AXES, None),
        P(None, AXES),
        P(AXES, None, None),
        P(AXES, None),
        P(),
        P(),
    )
    return jax.shard_map(
        local,
        mesh=mesh,
        in_specs=placed,
        out_specs=P(AXES, None, None),
        check_vma=False,
    )
```

```python
import math

import jax
import jax.numpy as jnp
from jax import lax
from jax.experimental import pallas as pl
from jax.experimental.pallas import tpu as pltpu
from jax.sharding import PartitionSpec as P

HEADS = 4
CAP = 8
QCAT = 8
LANES = 128
FINE = 8
BARRED = -1e30
MEBI = 1 << 20
AXES = ("role", "shard")


def iota(shape, dimension):
    return lax.broadcasted_iota(jnp.int32, shape, dimension)


def distinct_kernel(cat_ref, out_ref):
    cats = cat_ref[...].astype(jnp.float32)
    users = cats.shape[0]
    half = LANES // 2
    user = iota((users, LANES), 0)
    lane = iota((users, LANES), 1)
    beyond = jnp.float32(1e9)
    low = jnp.min(cats, axis=1, keepdims=True)
    high = jnp.max(cats, axis=1, keepdims=True)
    row = jnp.zeros((users, LANES), jnp.float32)
    for step in range(QCAT // 2):
        for place, value in ((step, low), (QCAT - 1 - step, high)):
            row = jnp.where(lane % half == place * users + user, value, row)
        if step + 1 < QCAT // 2:
            above = jnp.min(jnp.where(cats > low, cats, beyond), axis=1, keepdims=True)
            below = jnp.max(jnp.where(cats < high, cats, -beyond), axis=1, keepdims=True)
            low = jnp.where(above == beyond, low, above)
            high = jnp.where(below == -beyond, high, below)
    whole = jnp.sum(row, axis=0, keepdims=True).astype(jnp.int32)
    fine = whole & (FINE - 1)
    packed = jnp.where(iota((1, LANES), 1) < half, whole - fine, fine)
    out_ref[...] = jnp.broadcast_to(packed.reshape(1, 1, LANES), out_ref.shape)


def pack_kernel(wanted_ref, event_ref, history_ref, out_ref, *, own_users):
    devices = wanted_ref.shape[0]
    blocks_events = history_ref.shape[0]
    width = history_ref.shape[2]
    depth = event_ref.shape[1]
    span = depth // blocks_events
    per_group = span // own_users
    pairs = own_users // 2
    half = LANES // 2
    pad = -(-depth // LANES) * LANES
    wanted = wanted_ref[:, 0, :].astype(jnp.float32).astype(jnp.bfloat16)
    line = iota((LANES, pad), 0) % half
    mate = iota((LANES, pad), 1) % own_users
    events = event_ref[...].astype(jnp.float32)
    match = None
    for j in range(QCAT):
        spread = jnp.where(line == j * own_users + mate, 1.0, 0.0).astype(jnp.bfloat16)
        category = jnp.dot(wanted, spread, preferred_element_type=jnp.float32)[:, :depth]
        same = jnp.where(category == events, 1.0, 0.0)
        match = same if match is None else jnp.maximum(match, same)
    position = iota((devices, depth), 1) % span
    mine = position // own_users == iota((devices, depth), 0) % per_group
    match = jnp.where(mine, match, 0.0)
    before = iota((depth, pad), 0)
    here = iota((depth, pad), 1)
    user_before = before % span
    user_here = here % span
    counted = (user_before == user_here) & (before <= here)
    counted = counted | ((user_here % 2 == 1) & (user_before == user_here - 1))
    counted = jnp.where(counted, 1.0, 0.0).astype(jnp.bfloat16)
    matched = match.astype(jnp.bfloat16)
    place = jnp.dot(matched, counted, preferred_element_type=jnp.float32)[:, :depth]
    pair_base = ((position % own_users) // 2 * CAP - 1).astype(jnp.float32)
    code = jnp.where(match > 0.0, place + pair_base, -1.0)
    lane = iota((depth, LANES), 1)
    leading = (lane < pairs) & (iota((depth, LANES), 0) % own_users == 2 * lane)
    leading = jnp.where(leading, 1.0, 0.0).astype(jnp.bfloat16)
    lead = jnp.dot(matched, leading, preferred_element_type=jnp.float32)
    rows = pairs * CAP
    row = iota((rows, depth), 0).astype(jnp.float32)
    rank = iota((CAP, LANES), 0).astype(jnp.float32)
    for group in range(devices // per_group):
        stored = history_ref[:, group * span : (group + 1) * span, :].reshape(depth, width)
        picks = []
        for member in range(per_group):
            device = group * per_group + member
            picks.append(jnp.where(row == code[device : device + 1, :], 1.0, 0.0).astype(jnp.bfloat16))
        packed = jnp.dot(jnp.concatenate(picks, axis=0), stored, preferred_element_type=jnp.float32)
        packed = packed.astype(jnp.bfloat16)
        for member in range(per_group):
            device = group * per_group + member
            out_ref[device, :rows, :] = packed[member * rows : (member + 1) * rows, :]
            mark = jnp.where(rank < lead[device : device + 1, :], 1.0, 0.0)
            out_ref[device, rows:, :] = mark.astype(jnp.bfloat16)


def tower_kernel(packed_ref, cand_ref, w_in_ref, w_out_ref, out_ref):
    own_users, cand_count, width = cand_ref.shape
    pairs = own_users // 2
    devices = packed_ref.shape[0]
    slots = devices * CAP
    head_size = width // HEADS
    scale = math.log2(math.e) * head_size ** (-0.5)
    marks = packed_ref[:, pairs * CAP :, :].reshape(slots, LANES)
    pick = jnp.where(iota((2 * CAP, LANES), 0) == iota((2 * CAP, LANES), 1), 1.0, 0.0).astype(jnp.bfloat16)
    across = lax.dot_general(pick, marks, (((1,), (1,)), ((), ())), preferred_element_type=jnp.float32)
    marks = marks.astype(jnp.float32)
    slot_head = iota((slots, width), 1) // head_size
    head_of = iota((cand_count, width), 1) // head_size
    w_in = w_in_ref[...]
    w_out = w_out_ref[...]
    for pair in range(pairs):
        keys = packed_ref[:, pair * CAP : (pair + 1) * CAP, :].reshape(slots, width).astype(jnp.float32)
        owned = jnp.broadcast_to(marks[:, pair : pair + 1], (slots, width)) > 0.5
        own_keys = (jnp.where(owned, keys, 0.0), jnp.where(owned, 0.0, keys))
        ones = (jnp.where(owned, 1.0, 0.0), jnp.where(owned, 0.0, 1.0))
        right = jnp.concatenate([part.astype(jnp.bfloat16) for part in own_keys], axis=1)
        values = []
        for parity in range(2):
            mixed = [jnp.where(slot_head % 2 == parity, k, o).astype(jnp.bfloat16) for k, o in zip(own_keys, ones)]
            values.append(jnp.concatenate(mixed, axis=1))
        first = jnp.broadcast_to(across[pair : pair + 1, :], (cand_count, slots)) > 0.5
        cands = [cand_ref[2 * pair + member].astype(jnp.float32) for member in range(2)]
        tops = [jnp.zeros((cand_count, width), jnp.float32)] * 2
        totals = [jnp.ones((cand_count, width), jnp.float32)] * 2
        for head in range(HEADS):
            left = jnp.concatenate(
                [jnp.where(head_of == head, c, 0.0).astype(jnp.bfloat16) for c in cands], axis=1
            )
            scores = lax.dot_general(left, right, (((1,), (1,)), ((), ())), preferred_element_type=jnp.float32)
            peak_first = jnp.max(jnp.where(first, scores, BARRED), axis=1, keepdims=True)
            peak_second = jnp.max(jnp.where(first, BARRED, scores), axis=1, keepdims=True)
            expo = jnp.exp2((scores - jnp.where(first, peak_first, peak_second)) * scale).astype(jnp.bfloat16)
            both = jnp.dot(expo, values[head % 2], preferred_element_type=jnp.float32)
            for member in range(2):
                part = both[:, member * width : (member + 1) * width]
                tops[member] = jnp.where(head_of == head, part, tops[member])
                totals[member] = jnp.where(head_of == head ^ 1, part, totals[member])
        for member in range(2):
            inverse = 1.0 / totals[member]
            inverse = jnp.where(
                head_of % 2 == 0,
                pltpu.roll(inverse, width - head_size, 1),
                pltpu.roll(inverse, head_size, 1),
            )
            interest = (tops[member] * inverse).astype(jnp.bfloat16)
            joined = jnp.concatenate([cand_ref[2 * pair + member], interest], axis=1)
            hidden = jnp.dot(joined, w_in, preferred_element_type=jnp.float32)
            middle = hidden * 0.5
            hidden = (middle * jnp.tanh(middle) + middle).astype(jnp.bfloat16)
            result = jnp.dot(hidden, w_out, preferred_element_type=jnp.float32)
            out_ref[2 * pair + member] = result.astype(jnp.bfloat16)


def near(value):
    return pltpu.with_memory_space_constraint(value, pltpu.VMEM)


def exchange(parts):
    return lax.all_to_all(parts, AXES, split_axis=0, concat_axis=0, tiled=True)


def local(history, event_cat, candidates, cand_cat, w_input, w_output):
    devices = lax.axis_size(AXES)
    own_users, cand_count, width = candidates.shape
    users, block_events = event_cat.shape
    pairs = own_users // 2
    wanted = pl.pallas_call(
        distinct_kernel,
        out_shape=jax.ShapeDtypeStruct((devices, 1, LANES), jnp.int32),
        compiler_params=pltpu.CompilerParams(vmem_limit_bytes=4 * MEBI),
        name="distinct",
    )(cand_cat)
    wanted = exchange(wanted)
    resident = pl.BlockSpec(memory_space=pltpu.VMEM)
    span = math.lcm(16, own_users)
    grouped = event_cat.T.reshape(block_events, users // span, span).transpose(1, 0, 2)
    grouped = jnp.repeat(grouped.reshape(users // span, block_events * span), span // own_users, axis=0)
    packed = pl.pallas_call(
        lambda *refs: pack_kernel(*refs, own_users=own_users),
        out_shape=jax.ShapeDtypeStruct((devices, (pairs + 1) * CAP, width), jnp.bfloat16),
        in_specs=[resident] * 3,
        compiler_params=pltpu.CompilerParams(vmem_limit_bytes=24 * MEBI),
        name="pack",
    )(near(wanted), near(grouped), near(history.transpose(1, 0, 2)))
    received = exchange(packed)
    return pl.pallas_call(
        tower_kernel,
        out_shape=jax.ShapeDtypeStruct(candidates.shape, jnp.bfloat16),
        in_specs=[resident] * 4,
        compiler_params=pltpu.CompilerParams(vmem_limit_bytes=32 * MEBI),
        name="tower",
    )(near(received), near(candidates), near(w_input), near(w_output))


def solution(mesh):
    placed = (
        P(None, AXES, None),
        P(None, AXES),
        P(AXES, None, None),
        P(AXES, None),
        P(),
        P(),
    )
    return jax.shard_map(
        local,
        mesh=mesh,
        in_specs=placed,
        out_specs=P(AXES, None, None),
        check_vma=False,
    )
```

```python
import math

import jax
import jax.numpy as jnp
from jax import lax
from jax.experimental import pallas as pl
from jax.experimental.pallas import tpu as pltpu
from jax.sharding import PartitionSpec as P

HEADS = 4
CAP = 8
QCAT = 8
LANES = 128
FINE = 8
BARRED = -1e30
MEBI = 1 << 20
AXES = ("role", "shard")


def iota(shape, dimension):
    return lax.broadcasted_iota(jnp.int32, shape, dimension)


def distinct_kernel(cat_ref, out_ref):
    cats = cat_ref[...].astype(jnp.float32)
    users = cats.shape[0]
    half = LANES // 2
    user = iota((users, LANES), 0)
    lane = iota((users, LANES), 1)
    beyond = jnp.float32(1e9)
    low = jnp.min(cats, axis=1, keepdims=True)
    high = jnp.max(cats, axis=1, keepdims=True)
    row = jnp.zeros((users, LANES), jnp.float32)
    for step in range(QCAT // 2):
        for place, value in ((step, low), (QCAT - 1 - step, high)):
            row = jnp.where(lane % half == place * users + user, value, row)
        if step + 1 < QCAT // 2:
            above = jnp.min(jnp.where(cats > low, cats, beyond), axis=1, keepdims=True)
            below = jnp.max(jnp.where(cats < high, cats, -beyond), axis=1, keepdims=True)
            low = jnp.where(above == beyond, low, above)
            high = jnp.where(below == -beyond, high, below)
    whole = jnp.sum(row, axis=0, keepdims=True).astype(jnp.int32)
    fine = whole & (FINE - 1)
    packed = jnp.where(iota((1, LANES), 1) < half, whole - fine, fine)
    out_ref[...] = jnp.broadcast_to(packed.reshape(1, 1, LANES), out_ref.shape)


def pack_kernel(wanted_ref, event_ref, history_ref, query_ref, out_ref, *, own_users):
    del query_ref
    devices = wanted_ref.shape[0]
    blocks_events = history_ref.shape[0]
    width = history_ref.shape[2]
    depth = event_ref.shape[1]
    span = depth // blocks_events
    per_group = span // own_users
    pairs = own_users // 2
    half = LANES // 2
    pad = -(-depth // LANES) * LANES
    wanted = wanted_ref[:, 0, :].astype(jnp.float32).astype(jnp.bfloat16)
    line = iota((LANES, pad), 0) % half
    mate = iota((LANES, pad), 1) % own_users
    events = event_ref[...].astype(jnp.float32)
    match = None
    for j in range(QCAT):
        spread = jnp.where(line == j * own_users + mate, 1.0, 0.0).astype(jnp.bfloat16)
        category = jnp.dot(wanted, spread, preferred_element_type=jnp.float32)[:, :depth]
        same = jnp.where(category == events, 1.0, 0.0)
        match = same if match is None else jnp.maximum(match, same)
    position = iota((devices, depth), 1) % span
    mine = position // own_users == iota((devices, depth), 0) % per_group
    match = jnp.where(mine, match, 0.0)
    before = iota((depth, pad), 0)
    here = iota((depth, pad), 1)
    user_before = before % span
    user_here = here % span
    counted = (user_before == user_here) & (before <= here)
    counted = counted | ((user_here % 2 == 1) & (user_before == user_here - 1))
    counted = jnp.where(counted, 1.0, 0.0).astype(jnp.bfloat16)
    matched = match.astype(jnp.bfloat16)
    place = jnp.dot(matched, counted, preferred_element_type=jnp.float32)[:, :depth]
    pair_base = ((position % own_users) // 2 * CAP - 1).astype(jnp.float32)
    code = jnp.where(match > 0.0, place + pair_base, -1.0)
    lane = iota((depth, LANES), 1)
    leading = (lane < pairs) & (iota((depth, LANES), 0) % own_users == 2 * lane)
    leading = jnp.where(leading, 1.0, 0.0).astype(jnp.bfloat16)
    lead = jnp.dot(matched, leading, preferred_element_type=jnp.float32)
    rows = pairs * CAP
    row = iota((rows, depth), 0).astype(jnp.float32)
    rank = iota((CAP, LANES), 0).astype(jnp.float32)
    for group in range(devices // per_group):
        stored = history_ref[:, group * span : (group + 1) * span, :].reshape(depth, width)
        picks = []
        for member in range(per_group):
            device = group * per_group + member
            picks.append(jnp.where(row == code[device : device + 1, :], 1.0, 0.0).astype(jnp.bfloat16))
        packed = jnp.dot(jnp.concatenate(picks, axis=0), stored, preferred_element_type=jnp.float32)
        packed = packed.astype(jnp.bfloat16)
        for member in range(per_group):
            device = group * per_group + member
            out_ref[device, :rows, :] = packed[member * rows : (member + 1) * rows, :]
            mark = jnp.where(rank < lead[device : device + 1, :], 1.0, 0.0)
            out_ref[device, rows:, :] = mark.astype(jnp.bfloat16)


def stage_kernel(history_ref, staged_ref, sem):
    copy = pltpu.make_async_copy(history_ref, staged_ref, sem)
    copy.start()
    copy.wait()


def query_kernel(cand_ref, query_ref, *, cand_count):
    width = cand_ref.shape[1]
    head_of = iota((cand_count, width), 1) // (width // HEADS)
    for pair in range(query_ref.shape[0]):
        both = [
            cand_ref[(2 * pair + member) * cand_count : (2 * pair + member + 1) * cand_count, :].astype(jnp.float32)
            for member in range(2)
        ]
        for member in range(2):
            parts = [jnp.where(head_of == head, both[member], 0.0) for head in range(HEADS)]
            query_ref[pair, :, member * width : (member + 1) * width] = jnp.concatenate(parts, axis=0).astype(
                jnp.bfloat16
            )


def chunks(total, most):
    best = total
    for size in range(8, most + 1, 8):
        if total % size == 0 and (size % 16 == 0 or total % 16):
            best = size
    return [(start, best) for start in range(0, total, best)]


def tower_kernel(
    packed_ref, query_ref, cand_ref, w_in_ref, w_out_ref, out_ref,
    score_ref, weight_ref, sum_ref, interest_ref, hidden_ref, active_ref, result_ref, sems,
):
    pairs, head_rows, _ = query_ref.shape
    cand_count = head_rows // HEADS
    rows = 2 * cand_count
    width = cand_ref.shape[1]
    devices = packed_ref.shape[0]
    slots = devices * CAP
    head_size = width // HEADS
    scale = math.log2(math.e) * head_size ** (-0.5)
    marks = packed_ref[:, pairs * CAP :, :].reshape(slots, LANES)
    pick = jnp.where(iota((2 * CAP, LANES), 0) == iota((2 * CAP, LANES), 1), 1.0, 0.0).astype(jnp.bfloat16)
    across = lax.dot_general(pick, marks, (((1,), (1,)), ((), ())), preferred_element_type=jnp.float32)
    marks = marks.astype(jnp.float32)
    slot_even = (iota((slots, width), 1) // head_size) % 2 == 0
    values = {}

    def score(pair):
        keys = packed_ref[:, pair * CAP : (pair + 1) * CAP, :].reshape(slots, width).astype(jnp.float32)
        owned = jnp.broadcast_to(marks[:, pair : pair + 1], (slots, width))
        shared = 1.0 - owned
        own_keys = (keys * owned, keys * shared)
        right = jnp.concatenate([part.astype(jnp.bfloat16) for part in own_keys], axis=1)
        both = ((own_keys[0], owned), (own_keys[1], shared))
        values[pair] = (
            jnp.concatenate([jnp.where(slot_even, k, o).astype(jnp.bfloat16) for k, o in both], axis=1),
            jnp.concatenate([jnp.where(slot_even, o, k).astype(jnp.bfloat16) for k, o in both], axis=1),
        )
        score_ref[pair] = lax.dot_general(
            query_ref[pair], right, (((1,), (1,)), ((), ())), preferred_element_type=jnp.float32
        )

    def weigh(pair):
        mark = across[pair : pair + 1, :]
        bar_first = (1.0 - mark) * BARRED
        bar_second = mark * BARRED
        for start, size in chunks(head_rows, 32):
            scores = score_ref[pair, start : start + size, :]
            peak_first = jnp.max(scores + bar_first, axis=1, keepdims=True)
            peak_second = jnp.max(scores + bar_second, axis=1, keepdims=True)
            peak = jnp.where(mark > 0.5, peak_first, peak_second)
            weight_ref[pair, start : start + size, :] = jnp.exp2((scores - peak) * scale).astype(jnp.bfloat16)

    def gather(pair):
        for head in range(HEADS):
            span = slice(head * cand_count, (head + 1) * cand_count)
            sum_ref[pair, span, :] = jnp.dot(
                weight_ref[pair, span, :], values[pair][head % 2], preferred_element_type=jnp.float32
            )

    def blend(pair):
        for start, size in chunks(cand_count, 40):
            head_of = iota((size, width), 1) // head_size
            for member in range(2):
                parts = [
                    sum_ref[
                        pair,
                        head * cand_count + start : head * cand_count + start + size,
                        member * width : (member + 1) * width,
                    ]
                    for head in range(HEADS)
                ]
                top = parts[0]
                total = parts[HEADS - 1]
                for head in range(1, HEADS):
                    top = jnp.where(head_of == head, parts[head], top)
                    total = jnp.where(head_of == head, parts[head - 1], total)
                inverse = pltpu.roll(1.0 / total, width - head_size, 1)
                interest_ref[pair, member * cand_count + start : member * cand_count + start + size, :] = (
                    top * inverse
                )

    def enter(pair):
        joined = jnp.concatenate(
            [cand_ref[pair * rows : (pair + 1) * rows, :], interest_ref[pair].astype(jnp.bfloat16)], axis=1
        )
        hidden_ref[pair] = jnp.dot(joined, w_in_ref[...], preferred_element_type=jnp.float32)

    def activate(pair):
        for start, size in chunks(rows, 16):
            middle = hidden_ref[pair, start : start + size, :] * 0.5
            active_ref[pair, start : start + size, :] = (middle * jnp.tanh(middle) + middle).astype(jnp.bfloat16)

    def leave(pair):
        result = jnp.dot(active_ref[pair], w_out_ref[...], preferred_element_type=jnp.float32)
        result_ref[pair * rows : (pair + 1) * rows, :] = result.astype(jnp.bfloat16)
        copy_out(pair).start()

    def copy_out(pair):
        span = pl.ds(pair * rows, rows)
        return pltpu.make_async_copy(result_ref.at[span], out_ref.at[span], sems.at[pair])

    stages = (score, weigh, gather, blend, enter, activate, leave)
    lag = 2
    for tick in range(len(stages) + lag * (pairs - 1)):
        for pair in range(pairs):
            stage = tick - lag * pair
            if 0 <= stage < len(stages):
                stages[stage](pair)
    for pair in range(pairs):
        copy_out(pair).wait()


def near(value):
    return pltpu.with_memory_space_constraint(value, pltpu.VMEM)


def exchange(parts):
    return lax.all_to_all(parts, AXES, split_axis=0, concat_axis=0, tiled=True)


def local(history, event_cat, candidates, cand_cat, w_input, w_output):
    devices = lax.axis_size(AXES)
    own_users, cand_count, width = candidates.shape
    users, block_events = event_cat.shape
    pairs = own_users // 2
    resident = pl.BlockSpec(memory_space=pltpu.VMEM)
    wanted = pl.pallas_call(
        distinct_kernel,
        out_shape=pltpu.VMEM((devices, 1, LANES), jnp.int32),
        out_specs=resident,
        compiler_params=pltpu.CompilerParams(vmem_limit_bytes=4 * MEBI),
        name="distinct",
    )(cand_cat)
    wanted = exchange(wanted)
    by_event = history.transpose(1, 0, 2)
    stored = pl.pallas_call(
        stage_kernel,
        out_shape=pltpu.VMEM(by_event.shape, jnp.bfloat16),
        in_specs=[pl.BlockSpec(memory_space=pltpu.HBM)],
        out_specs=resident,
        scratch_shapes=[pltpu.SemaphoreType.DMA(())],
        compiler_params=pltpu.CompilerParams(vmem_limit_bytes=4 * MEBI),
        name="stage",
    )(by_event)
    rows = own_users * cand_count
    queries = near(candidates.reshape(rows, width))
    query = pl.pallas_call(
        lambda *refs: query_kernel(*refs, cand_count=cand_count),
        out_shape=pltpu.VMEM((pairs, HEADS * cand_count, 2 * width), jnp.bfloat16),
        in_specs=[resident],
        out_specs=resident,
        compiler_params=pltpu.CompilerParams(vmem_limit_bytes=16 * MEBI),
        name="query",
    )(queries)
    span = math.lcm(16, own_users)
    grouped = event_cat.T.reshape(block_events, users // span, span).transpose(1, 0, 2)
    grouped = jnp.repeat(grouped.reshape(users // span, block_events * span), span // own_users, axis=0)
    packed = pl.pallas_call(
        lambda *refs: pack_kernel(*refs, own_users=own_users),
        out_shape=pltpu.VMEM((devices, (pairs + 1) * CAP, width), jnp.bfloat16),
        out_specs=resident,
        in_specs=[resident] * 4,
        compiler_params=pltpu.CompilerParams(vmem_limit_bytes=24 * MEBI),
        name="pack",
    )(near(wanted), near(grouped), near(stored), near(query))
    received = exchange(packed)
    slots = devices * CAP
    result = pl.pallas_call(
        tower_kernel,
        out_shape=jax.ShapeDtypeStruct((rows, width), jnp.bfloat16),
        in_specs=[resident] * 5,
        out_specs=pl.BlockSpec(memory_space=pltpu.HBM),
        scratch_shapes=[
            pltpu.VMEM((pairs, HEADS * cand_count, slots), jnp.float32),
            pltpu.VMEM((pairs, HEADS * cand_count, slots), jnp.bfloat16),
            pltpu.VMEM((pairs, HEADS * cand_count, 2 * width), jnp.float32),
            pltpu.VMEM((pairs, 2 * cand_count, width), jnp.float32),
            pltpu.VMEM((pairs, 2 * cand_count, w_input.shape[1]), jnp.float32),
            pltpu.VMEM((pairs, 2 * cand_count, w_input.shape[1]), jnp.bfloat16),
            pltpu.VMEM((rows, width), jnp.bfloat16),
            pltpu.SemaphoreType.DMA((pairs,)),
        ],
        compiler_params=pltpu.CompilerParams(vmem_limit_bytes=40 * MEBI),
        name="tower",
    )(near(received), near(query), queries, near(w_input), near(w_output))
    return result.reshape(own_users, cand_count, width)


def solution(mesh):
    placed = (
        P(None, AXES, None),
        P(None, AXES),
        P(AXES, None, None),
        P(AXES, None),
        P(),
        P(),
    )
    return jax.shard_map(
        local,
        mesh=mesh,
        in_specs=placed,
        out_specs=P(AXES, None, None),
        check_vma=False,
    )
```

```python
import math

import jax
import jax.numpy as jnp
from jax import lax
from jax.experimental import pallas as pl
from jax.experimental.pallas import tpu as pltpu
from jax.sharding import PartitionSpec as P

HEADS = 4
CAP = 8
QCAT = 8
LANES = 128
FINE = 8
BARRED = -1e30
MEBI = 1 << 20
STREAMS = 5
AXES = ("role", "shard")


def iota(shape, dimension):
    return lax.broadcasted_iota(jnp.int32, shape, dimension)


def distinct_kernel(cat_ref, out_ref):
    cats = cat_ref[...].astype(jnp.float32)
    users = cats.shape[0]
    half = LANES // 2
    user = iota((users, LANES), 0)
    lane = iota((users, LANES), 1)
    beyond = jnp.float32(1e9)
    low = jnp.min(cats, axis=1, keepdims=True)
    high = jnp.max(cats, axis=1, keepdims=True)
    row = jnp.zeros((users, LANES), jnp.float32)
    for step in range(QCAT // 2):
        for place, value in ((step, low), (QCAT - 1 - step, high)):
            row = jnp.where(lane % half == place * users + user, value, row)
        if step + 1 < QCAT // 2:
            above = jnp.min(jnp.where(cats > low, cats, beyond), axis=1, keepdims=True)
            below = jnp.max(jnp.where(cats < high, cats, -beyond), axis=1, keepdims=True)
            low = jnp.where(above == beyond, low, above)
            high = jnp.where(below == -beyond, high, below)
    whole = jnp.sum(row, axis=0, keepdims=True).astype(jnp.int32)
    fine = whole & (FINE - 1)
    packed = jnp.where(iota((1, LANES), 1) < half, whole - fine, fine)
    out_ref[...] = jnp.broadcast_to(packed.reshape(1, 1, LANES), out_ref.shape)


def pack_kernel(wanted_ref, event_ref, history_ref, out_ref, *, own_users):
    devices = wanted_ref.shape[0]
    blocks_events = history_ref.shape[0]
    width = history_ref.shape[2]
    depth = event_ref.shape[1]
    span = depth // blocks_events
    per_group = span // own_users
    pairs = own_users // 2
    half = LANES // 2
    pad = -(-depth // LANES) * LANES
    wanted = wanted_ref[:, 0, :].astype(jnp.float32).astype(jnp.bfloat16)
    line = iota((LANES, pad), 0) % half
    mate = iota((LANES, pad), 1) % own_users
    events = event_ref[...]
    match = None
    for j in range(QCAT):
        spread = jnp.where(line == j * own_users + mate, 1.0, 0.0).astype(jnp.bfloat16)
        category = jnp.dot(wanted, spread, preferred_element_type=jnp.float32)[:, :depth]
        same = jnp.where(category == events, 1.0, 0.0)
        match = same if match is None else jnp.maximum(match, same)
    position = iota((devices, depth), 1) % span
    before = iota((depth, pad), 0)
    here = iota((depth, pad), 1)
    user_before = before % span
    user_here = here % span
    counted = (user_before == user_here) & (before <= here)
    counted = counted | ((user_here % 2 == 1) & (user_before == user_here - 1))
    counted = jnp.where(counted, 1.0, 0.0).astype(jnp.bfloat16)
    matched = match.astype(jnp.bfloat16)
    place = jnp.dot(matched, counted, preferred_element_type=jnp.float32)[:, :depth]
    pair_base = ((position % own_users) // 2 * CAP - 1).astype(jnp.float32)
    code = jnp.where(match > 0.0, place + pair_base, -1.0)
    lane = iota((depth, LANES), 1)
    leading = (lane < pairs) & (iota((depth, LANES), 0) % own_users == 2 * lane)
    leading = jnp.where(leading, 1.0, 0.0).astype(jnp.bfloat16)
    lead = jnp.dot(matched, leading, preferred_element_type=jnp.float32)
    rows = pairs * CAP
    row = iota((rows, depth), 0).astype(jnp.float32)
    rank = iota((CAP, LANES), 0).astype(jnp.float32)
    for group in range(devices // per_group):
        stored = history_ref[:, group * span : (group + 1) * span, :].reshape(depth, width)
        picks = []
        for member in range(per_group):
            device = group * per_group + member
            picks.append(jnp.where(row == code[device : device + 1, :], 1.0, 0.0).astype(jnp.bfloat16))
        packed = jnp.dot(jnp.concatenate(picks, axis=0), stored, preferred_element_type=jnp.float32)
        packed = packed.astype(jnp.bfloat16)
        for member in range(per_group):
            device = group * per_group + member
            out_ref[device, :rows, :] = packed[member * rows : (member + 1) * rows, :]
            mark = jnp.where(rank < lead[device : device + 1, :], 1.0, 0.0)
            out_ref[device, rows:, :] = mark.astype(jnp.bfloat16)


def stage_kernel(
    history_ref, cand_ref, event_ref, stored_ref, query_ref, grouped_ref, cand_scratch, event_scratch, sems, *, own_users
):
    event_copy = pltpu.make_async_copy(event_ref, event_scratch, sems.at[0])
    cand_copy = pltpu.make_async_copy(cand_ref, cand_scratch, sems.at[1])
    events = history_ref.shape[0]
    cuts = [events * part // STREAMS for part in range(STREAMS + 1)]
    history_copies = [
        pltpu.make_async_copy(
            history_ref.at[pl.ds(low, high - low)], stored_ref.at[pl.ds(low, high - low)], sems.at[2 + part]
        )
        for part, (low, high) in enumerate(zip(cuts, cuts[1:]))
    ]
    event_copy.start()
    cand_copy.start()
    for copy in history_copies:
        copy.start()

    event_copy.wait()
    users = event_ref.shape[1]
    devices = users // own_users
    depth = grouped_ref.shape[1]
    span = depth // events
    fold = LANES // span
    owner = iota((devices, users), 1) // own_users == iota((devices, users), 0)
    parts = ([], [])
    for event in range(events):
        line = event_scratch[event : event + 1, :]
        fine = line & (FINE - 1)
        for part, value in zip(parts, (line - fine, fine)):
            part.append(jnp.where(owner, value.astype(jnp.float32), 0.0).astype(jnp.bfloat16))
    spread = jnp.where(iota((users, LANES), 0) % span == iota((users, LANES), 1) % span, 1.0, 0.0).astype(jnp.bfloat16)
    picked = sum(
        jnp.dot(jnp.concatenate(part, axis=0), spread, preferred_element_type=jnp.float32) for part in parts
    )
    lane = iota((devices, LANES), 1)
    mine = lane % span // own_users == iota((devices, LANES), 0) % (span // own_users)
    for first in range(0, events, fold):
        tile = jnp.full((devices, LANES), -1.0, jnp.float32)
        for event in range(first, min(first + fold, events)):
            rows = picked[event * devices : (event + 1) * devices, :]
            tile = jnp.where(mine & (lane // span == event - first), rows, tile)
        low = first * span
        high = min(low + LANES, depth)
        grouped_ref[:, low:high] = tile[:, : high - low]

    cand_copy.wait()
    width = cand_ref.shape[1]
    cand_count = query_ref.shape[1] // HEADS
    head_of = iota((cand_count, width), 1) // (width // HEADS)
    for pair in range(query_ref.shape[0]):
        for member in range(2):
            start = (2 * pair + member) * cand_count
            cands = cand_scratch[start : start + cand_count, :].astype(jnp.float32)
            heads = [jnp.where(head_of == head, cands, 0.0) for head in range(HEADS)]
            query_ref[pair, :, member * width : (member + 1) * width] = jnp.concatenate(heads, axis=0).astype(
                jnp.bfloat16
            )
    for copy in history_copies:
        copy.wait()


def chunks(total, most):
    best = total
    for size in range(8, most + 1, 8):
        if total % size == 0 and (size % 16 == 0 or total % 16):
            best = size
    return [(start, best) for start in range(0, total, best)]


def tower_kernel(
    packed_ref, query_ref, cand_ref, w_in_ref, w_out_ref, out_ref,
    score_ref, weight_ref, sum_ref, interest_ref, hidden_ref, active_ref, result_ref, sems,
):
    pairs, head_rows, _ = query_ref.shape
    cand_count = head_rows // HEADS
    rows = 2 * cand_count
    width = cand_ref.shape[1]
    devices = packed_ref.shape[0]
    slots = devices * CAP
    head_size = width // HEADS
    scale = math.log2(math.e) * head_size ** (-0.5)
    marks = packed_ref[:, pairs * CAP :, :].reshape(slots, LANES)
    pick = jnp.where(iota((2 * CAP, LANES), 0) == iota((2 * CAP, LANES), 1), 1.0, 0.0).astype(jnp.bfloat16)
    across = lax.dot_general(pick, marks, (((1,), (1,)), ((), ())), preferred_element_type=jnp.float32)
    marks = marks.astype(jnp.float32)
    slot_even = (iota((slots, width), 1) // head_size) % 2 == 0
    values = {}

    def score(pair):
        keys = packed_ref[:, pair * CAP : (pair + 1) * CAP, :].reshape(slots, width).astype(jnp.float32)
        owned = jnp.broadcast_to(marks[:, pair : pair + 1], (slots, width))
        shared = 1.0 - owned
        own_keys = (keys * owned, keys * shared)
        right = jnp.concatenate([part.astype(jnp.bfloat16) for part in own_keys], axis=1)
        both = ((own_keys[0], owned), (own_keys[1], shared))
        values[pair] = (
            jnp.concatenate([jnp.where(slot_even, k, o).astype(jnp.bfloat16) for k, o in both], axis=1),
            jnp.concatenate([jnp.where(slot_even, o, k).astype(jnp.bfloat16) for k, o in both], axis=1),
        )
        score_ref[pair] = lax.dot_general(
            query_ref[pair], right, (((1,), (1,)), ((), ())), preferred_element_type=jnp.float32
        )

    def weigh(pair):
        mark = across[pair : pair + 1, :]
        bar_first = (1.0 - mark) * BARRED
        bar_second = mark * BARRED
        for start, size in chunks(head_rows, 32):
            scores = score_ref[pair, start : start + size, :]
            peak_first = jnp.max(scores + bar_first, axis=1, keepdims=True)
            peak_second = jnp.max(scores + bar_second, axis=1, keepdims=True)
            peak = jnp.where(mark > 0.5, peak_first, peak_second)
            weight_ref[pair, start : start + size, :] = jnp.exp2((scores - peak) * scale).astype(jnp.bfloat16)

    def gather(pair):
        for head in range(HEADS):
            span = slice(head * cand_count, (head + 1) * cand_count)
            sum_ref[pair, span, :] = jnp.dot(
                weight_ref[pair, span, :], values[pair][head % 2], preferred_element_type=jnp.float32
            )

    def blend(pair):
        for start, size in chunks(cand_count, 40):
            head_of = iota((size, width), 1) // head_size
            for member in range(2):
                parts = [
                    sum_ref[
                        pair,
                        head * cand_count + start : head * cand_count + start + size,
                        member * width : (member + 1) * width,
                    ]
                    for head in range(HEADS)
                ]
                top = parts[0]
                total = parts[HEADS - 1]
                for head in range(1, HEADS):
                    top = jnp.where(head_of == head, parts[head], top)
                    total = jnp.where(head_of == head, parts[head - 1], total)
                inverse = pltpu.roll(1.0 / total, width - head_size, 1)
                interest_ref[pair, member * cand_count + start : member * cand_count + start + size, :] = (
                    top * inverse
                )

    def enter(pair):
        joined = jnp.concatenate(
            [cand_ref[pair * rows : (pair + 1) * rows, :], interest_ref[pair].astype(jnp.bfloat16)], axis=1
        )
        hidden_ref[pair] = jnp.dot(joined, w_in_ref[...], preferred_element_type=jnp.float32)

    def activate(pair):
        for start, size in chunks(rows, 16):
            middle = hidden_ref[pair, start : start + size, :] * 0.5
            active_ref[pair, start : start + size, :] = (middle * jnp.tanh(middle) + middle).astype(jnp.bfloat16)

    def leave(pair):
        result = jnp.dot(active_ref[pair], w_out_ref[...], preferred_element_type=jnp.float32)
        result_ref[pair * rows : (pair + 1) * rows, :] = result.astype(jnp.bfloat16)
        copy_out(pair).start()

    def copy_out(pair):
        span = pl.ds(pair * rows, rows)
        return pltpu.make_async_copy(result_ref.at[span], out_ref.at[span], sems.at[pair])

    stages = (score, weigh, gather, blend, enter, activate, leave)
    lag = 2
    for tick in range(len(stages) + lag * (pairs - 1)):
        for pair in range(pairs):
            stage = tick - lag * pair
            if 0 <= stage < len(stages):
                stages[stage](pair)
    for pair in range(pairs):
        copy_out(pair).wait()


def near(value):
    return pltpu.with_memory_space_constraint(value, pltpu.VMEM)


def exchange(parts):
    return lax.all_to_all(parts, AXES, split_axis=0, concat_axis=0, tiled=True)


def local(history, event_cat, candidates, cand_cat, w_input, w_output):
    devices = lax.axis_size(AXES)
    own_users, cand_count, width = candidates.shape
    users, block_events = event_cat.shape
    pairs = own_users // 2
    resident = pl.BlockSpec(memory_space=pltpu.VMEM)
    wanted = pl.pallas_call(
        distinct_kernel,
        out_shape=pltpu.VMEM((devices, 1, LANES), jnp.int32),
        out_specs=resident,
        compiler_params=pltpu.CompilerParams(vmem_limit_bytes=4 * MEBI),
        name="distinct",
    )(cand_cat)
    wanted = exchange(wanted)
    by_event = history.transpose(1, 0, 2)
    rows = own_users * cand_count
    flat_cands = candidates.reshape(rows, width)
    span = math.lcm(16, own_users)
    far = pl.BlockSpec(memory_space=pltpu.HBM)
    stored, query, grouped = pl.pallas_call(
        lambda *refs: stage_kernel(*refs, own_users=own_users),
        out_shape=[
            pltpu.VMEM(by_event.shape, jnp.bfloat16),
            pltpu.VMEM((pairs, HEADS * cand_count, 2 * width), jnp.bfloat16),
            pltpu.VMEM((devices, block_events * span), jnp.float32),
        ],
        in_specs=[far] * 3,
        out_specs=[resident] * 3,
        scratch_shapes=[
            pltpu.VMEM((rows, width), jnp.bfloat16),
            pltpu.VMEM((block_events, users), jnp.int32),
            pltpu.SemaphoreType.DMA((2 + STREAMS,)),
        ],
        compiler_params=pltpu.CompilerParams(vmem_limit_bytes=24 * MEBI),
        name="stage",
    )(*[pltpu.with_memory_space_constraint(value, pltpu.HBM) for value in (by_event, flat_cands, event_cat.T)])
    packed = pl.pallas_call(
        lambda *refs: pack_kernel(*refs, own_users=own_users),
        out_shape=pltpu.VMEM((devices, (pairs + 1) * CAP, width), jnp.bfloat16),
        out_specs=resident,
        in_specs=[resident] * 3,
        compiler_params=pltpu.CompilerParams(vmem_limit_bytes=24 * MEBI),
        name="pack",
    )(near(wanted), near(grouped), near(stored))
    received = exchange(packed)
    slots = devices * CAP
    result = pl.pallas_call(
        tower_kernel,
        out_shape=jax.ShapeDtypeStruct((rows, width), jnp.bfloat16),
        in_specs=[resident] * 5,
        out_specs=pl.BlockSpec(memory_space=pltpu.HBM),
        scratch_shapes=[
            pltpu.VMEM((pairs, HEADS * cand_count, slots), jnp.float32),
            pltpu.VMEM((pairs, HEADS * cand_count, slots), jnp.bfloat16),
            pltpu.VMEM((pairs, HEADS * cand_count, 2 * width), jnp.float32),
            pltpu.VMEM((pairs, 2 * cand_count, width), jnp.float32),
            pltpu.VMEM((pairs, 2 * cand_count, w_input.shape[1]), jnp.float32),
            pltpu.VMEM((pairs, 2 * cand_count, w_input.shape[1]), jnp.bfloat16),
            pltpu.VMEM((rows, width), jnp.bfloat16),
            pltpu.SemaphoreType.DMA((pairs,)),
        ],
        compiler_params=pltpu.CompilerParams(vmem_limit_bytes=40 * MEBI),
        name="tower",
    )(near(received), near(query), near(flat_cands), near(w_input), near(w_output))
    return result.reshape(own_users, cand_count, width)


def solution(mesh):
    placed = (
        P(None, AXES, None),
        P(None, AXES),
        P(AXES, None, None),
        P(AXES, None),
        P(),
        P(),
    )
    return jax.shard_map(
        local,
        mesh=mesh,
        in_specs=placed,
        out_specs=P(AXES, None, None),
        check_vma=False,
    )
```

```python
import math

import jax
import jax.numpy as jnp
from jax import lax
from jax.experimental import pallas as pl
from jax.experimental.pallas import tpu as pltpu
from jax.sharding import PartitionSpec as P

HEADS = 4
CAP = 8
QCAT = 8
LANES = 128
FINE = 8
HEAD_ORDER = (*range(0, HEADS, 2), *range(1, HEADS, 2))
BARRED = -1e30
MEBI = 1 << 20
STREAMS = 5
AXES = ("role", "shard")


def iota(shape, dimension):
    return lax.broadcasted_iota(jnp.int32, shape, dimension)


def distinct_kernel(cat_ref, out_ref):
    cats = cat_ref[...].astype(jnp.float32)
    users = cats.shape[0]
    half = LANES // 2
    user = iota((users, LANES), 0)
    lane = iota((users, LANES), 1)
    beyond = jnp.float32(1e9)
    low = jnp.min(cats, axis=1, keepdims=True)
    high = jnp.max(cats, axis=1, keepdims=True)
    row = jnp.zeros((users, LANES), jnp.float32)
    for step in range(QCAT // 2):
        for place, value in ((step, low), (QCAT - 1 - step, high)):
            row = jnp.where(lane % half == place * users + user, value, row)
        if step + 1 < QCAT // 2:
            above = jnp.min(jnp.where(cats > low, cats, beyond), axis=1, keepdims=True)
            below = jnp.max(jnp.where(cats < high, cats, -beyond), axis=1, keepdims=True)
            low = jnp.where(above == beyond, low, above)
            high = jnp.where(below == -beyond, high, below)
    whole = jnp.sum(row, axis=0, keepdims=True).astype(jnp.int32)
    fine = whole & (FINE - 1)
    packed = jnp.where(iota((1, LANES), 1) < half, whole - fine, fine)
    out_ref[...] = jnp.broadcast_to(packed.reshape(1, 1, LANES), out_ref.shape)


def pack_kernel(wanted_ref, event_ref, history_ref, out_ref, *, own_users):
    devices = wanted_ref.shape[0]
    blocks_events = history_ref.shape[0]
    width = history_ref.shape[2]
    depth = event_ref.shape[1]
    span = depth // blocks_events
    per_group = span // own_users
    pairs = own_users // 2
    half = LANES // 2
    pad = -(-depth // LANES) * LANES
    wanted = wanted_ref[:, 0, :].astype(jnp.float32).astype(jnp.bfloat16)
    line = iota((LANES, pad), 0) % half
    mate = iota((LANES, pad), 1) % own_users
    events = event_ref[...]
    match = None
    for j in range(QCAT):
        spread = jnp.where(line == j * own_users + mate, 1.0, 0.0).astype(jnp.bfloat16)
        category = jnp.dot(wanted, spread, preferred_element_type=jnp.float32)[:, :depth]
        same = jnp.where(category == events, 1.0, 0.0)
        match = same if match is None else jnp.maximum(match, same)
    position = iota((devices, depth), 1) % span
    before = iota((depth, pad), 0)
    here = iota((depth, pad), 1)
    user_before = before % span
    user_here = here % span
    counted = (user_before == user_here) & (before <= here)
    counted = counted | ((user_here % 2 == 1) & (user_before == user_here - 1))
    counted = jnp.where(counted, 1.0, 0.0).astype(jnp.bfloat16)
    matched = match.astype(jnp.bfloat16)
    place = jnp.dot(matched, counted, preferred_element_type=jnp.float32)[:, :depth]
    pair_base = ((position % own_users) // 2 * CAP - 1).astype(jnp.float32)
    code = jnp.where(match > 0.0, place + pair_base, -1.0)
    lane = iota((depth, LANES), 1)
    leading = (lane < pairs) & (iota((depth, LANES), 0) % own_users == 2 * lane)
    leading = jnp.where(leading, 1.0, 0.0).astype(jnp.bfloat16)
    lead = jnp.dot(matched, leading, preferred_element_type=jnp.float32)
    rows = pairs * CAP
    row = iota((rows, depth), 0).astype(jnp.float32)
    rank = iota((CAP, LANES), 0).astype(jnp.float32)
    for group in range(devices // per_group):
        stored = history_ref[:, group * span : (group + 1) * span, :].reshape(depth, width)
        picks = []
        for member in range(per_group):
            device = group * per_group + member
            picks.append(jnp.where(row == code[device : device + 1, :], 1.0, 0.0).astype(jnp.bfloat16))
        packed = jnp.dot(jnp.concatenate(picks, axis=0), stored, preferred_element_type=jnp.float32)
        packed = packed.astype(jnp.bfloat16)
        for member in range(per_group):
            device = group * per_group + member
            out_ref[device, :rows, :] = packed[member * rows : (member + 1) * rows, :]
            mark = jnp.where(rank < lead[device : device + 1, :], 1.0, 0.0)
            out_ref[device, rows:, :] = mark.astype(jnp.bfloat16)


def stage_kernel(
    history_ref, cand_ref, event_ref, stored_ref, query_ref, grouped_ref, cand_scratch, event_scratch, sems, *, own_users
):
    event_copy = pltpu.make_async_copy(event_ref, event_scratch, sems.at[0])
    cand_copy = pltpu.make_async_copy(cand_ref, cand_scratch, sems.at[1])
    events = history_ref.shape[0]
    cuts = [events * part // STREAMS for part in range(STREAMS + 1)]
    history_copies = [
        pltpu.make_async_copy(
            history_ref.at[pl.ds(low, high - low)], stored_ref.at[pl.ds(low, high - low)], sems.at[2 + part]
        )
        for part, (low, high) in enumerate(zip(cuts, cuts[1:]))
    ]
    event_copy.start()
    cand_copy.start()
    for copy in history_copies:
        copy.start()

    event_copy.wait()
    users = event_ref.shape[1]
    devices = users // own_users
    depth = grouped_ref.shape[1]
    span = depth // events
    fold = LANES // span
    owner = iota((devices, users), 1) // own_users == iota((devices, users), 0)
    parts = ([], [])
    for event in range(events):
        line = event_scratch[event : event + 1, :]
        fine = line & (FINE - 1)
        for part, value in zip(parts, (line - fine, fine)):
            part.append(jnp.where(owner, value.astype(jnp.float32), 0.0).astype(jnp.bfloat16))
    spread = jnp.where(iota((users, LANES), 0) % span == iota((users, LANES), 1) % span, 1.0, 0.0).astype(jnp.bfloat16)
    picked = sum(
        jnp.dot(jnp.concatenate(part, axis=0), spread, preferred_element_type=jnp.float32) for part in parts
    )
    lane = iota((devices, LANES), 1)
    mine = lane % span // own_users == iota((devices, LANES), 0) % (span // own_users)
    for first in range(0, events, fold):
        tile = jnp.full((devices, LANES), -1.0, jnp.float32)
        for event in range(first, min(first + fold, events)):
            rows = picked[event * devices : (event + 1) * devices, :]
            tile = jnp.where(mine & (lane // span == event - first), rows, tile)
        low = first * span
        high = min(low + LANES, depth)
        grouped_ref[:, low:high] = tile[:, : high - low]

    cand_copy.wait()
    width = cand_ref.shape[1]
    cand_count = query_ref.shape[1] // HEADS
    head_of = iota((cand_count, width), 1) // (width // HEADS)
    for pair in range(query_ref.shape[0]):
        for member in range(2):
            start = (2 * pair + member) * cand_count
            cands = cand_scratch[start : start + cand_count, :].astype(jnp.float32)
            heads = [jnp.where(head_of == head, cands, 0.0) for head in HEAD_ORDER]
            query_ref[pair, :, member * width : (member + 1) * width] = jnp.concatenate(heads, axis=0).astype(
                jnp.bfloat16
            )
    for copy in history_copies:
        copy.wait()


def chunks(total, most):
    best = total
    for size in range(8, most + 1, 8):
        if total % size == 0 and (size % 16 == 0 or total % 16):
            best = size
    return [(start, best) for start in range(0, total, best)]


def tower_kernel(
    packed_ref, query_ref, cand_ref, w_in_ref, w_out_ref, out_ref,
    score_ref, weight_ref, sum_ref, interest_ref, hidden_ref, active_ref, half_ref, result_ref, sems,
):
    pairs, head_rows, _ = query_ref.shape
    cand_count = head_rows // HEADS
    rows = 2 * cand_count
    width = cand_ref.shape[1]
    devices = packed_ref.shape[0]
    slots = devices * CAP
    head_size = width // HEADS
    scale = math.log2(math.e) * head_size ** (-0.5)
    marks = packed_ref[:, pairs * CAP :, :].reshape(slots, LANES)
    pick = jnp.where(iota((2 * CAP, LANES), 0) == iota((2 * CAP, LANES), 1), 1.0, 0.0).astype(jnp.bfloat16)
    across = lax.dot_general(pick, marks, (((1,), (1,)), ((), ())), preferred_element_type=jnp.float32)
    marks = marks.astype(jnp.float32)
    slot_even = ((iota((slots, width), 1) // head_size) % 2).astype(jnp.float32).astype(jnp.bfloat16) == 0
    values = {}
    half_ref[...] = w_in_ref[...] * 0.5

    def score(pair):
        keys = packed_ref[:, pair * CAP : (pair + 1) * CAP, :].reshape(slots, width)
        owned = jnp.broadcast_to(marks[:, pair : pair + 1], (slots, width)).astype(jnp.bfloat16)
        shared = 1 - owned
        own_keys = (keys * owned, keys * shared)
        right = jnp.concatenate(own_keys, axis=1)
        both = ((own_keys[0], owned), (own_keys[1], shared))
        values[pair] = (
            jnp.concatenate([jnp.where(slot_even, k, o) for k, o in both], axis=1),
            jnp.concatenate([jnp.where(slot_even, o, k) for k, o in both], axis=1),
        )
        score_ref[pair] = lax.dot_general(
            query_ref[pair], right, (((1,), (1,)), ((), ())), preferred_element_type=jnp.float32
        )

    def weigh(pair):
        mark = across[pair : pair + 1, :]
        bar_first = ((1.0 - mark) * BARRED).astype(jnp.bfloat16)
        bar_second = (mark * BARRED).astype(jnp.bfloat16)
        for start, size in chunks(head_rows, 160):
            scores = score_ref[pair, start : start + size, :]
            rough = scores.astype(jnp.bfloat16)
            peak_first = jnp.max(rough + bar_first, axis=1, keepdims=True).astype(jnp.float32)
            peak_second = jnp.max(rough + bar_second, axis=1, keepdims=True).astype(jnp.float32)
            peak = jnp.where(mark > 0.5, peak_first, peak_second)
            weight_ref[pair, start : start + size, :] = jnp.exp2((scores - peak) * scale).astype(jnp.bfloat16)

    def gather(pair):
        for block, head in enumerate(HEAD_ORDER):
            span = slice(block * cand_count, (block + 1) * cand_count)
            sum_ref[pair, span, :] = jnp.dot(
                weight_ref[pair, span, :], values[pair][head % 2], preferred_element_type=jnp.float32
            )

    def blend(pair):
        for start, size in chunks(cand_count, 40):
            head_of = iota((size, width), 1) // head_size
            for member in range(2):
                parts = [
                    sum_ref[
                        pair,
                        block * cand_count + start : block * cand_count + start + size,
                        member * width : (member + 1) * width,
                    ]
                    for block in map(HEAD_ORDER.index, range(HEADS))
                ]
                top = parts[0]
                total = parts[HEADS - 1]
                for head in range(1, HEADS):
                    top = jnp.where(head_of == head, parts[head], top)
                    total = jnp.where(head_of == head, parts[head - 1], total)
                inverse = pltpu.roll(1.0 / total, width - head_size, 1)
                interest_ref[pair, member * cand_count + start : member * cand_count + start + size, :] = (
                    top * inverse
                )

    def enter(pair):
        joined = jnp.concatenate(
            [cand_ref[pair * rows : (pair + 1) * rows, :], interest_ref[pair].astype(jnp.bfloat16)], axis=1
        )
        hidden_ref[pair] = jnp.dot(joined, half_ref[...], preferred_element_type=jnp.float32)

    def activate(pair):
        for start, size in chunks(rows, 16):
            middle = hidden_ref[pair, start : start + size, :]
            active_ref[pair, start : start + size, :] = (middle * jnp.tanh(middle) + middle).astype(jnp.bfloat16)

    def leave(pair):
        result = jnp.dot(active_ref[pair], w_out_ref[...], preferred_element_type=jnp.float32)
        result_ref[pair * rows : (pair + 1) * rows, :] = result.astype(jnp.bfloat16)
        copy_out(pair).start()

    def copy_out(pair):
        span = pl.ds(pair * rows, rows)
        return pltpu.make_async_copy(result_ref.at[span], out_ref.at[span], sems.at[pair])

    stages = (score, weigh, gather, blend, enter, activate, leave)
    begins = [pair // 2 * 5 for pair in range(pairs)]
    for tick in range(len(stages) + begins[-1]):
        for pair in range(pairs):
            stage = tick - begins[pair]
            if 0 <= stage < len(stages):
                stages[stage](pair)
    for pair in range(pairs):
        copy_out(pair).wait()


def near(value):
    return pltpu.with_memory_space_constraint(value, pltpu.VMEM)


def exchange(parts):
    return lax.all_to_all(parts, AXES, split_axis=0, concat_axis=0, tiled=True)


def local(history, event_cat, candidates, cand_cat, w_input, w_output):
    devices = lax.axis_size(AXES)
    own_users, cand_count, width = candidates.shape
    users, block_events = event_cat.shape
    pairs = own_users // 2
    resident = pl.BlockSpec(memory_space=pltpu.VMEM)
    wanted = pl.pallas_call(
        distinct_kernel,
        out_shape=pltpu.VMEM((devices, 1, LANES), jnp.int32),
        out_specs=resident,
        compiler_params=pltpu.CompilerParams(vmem_limit_bytes=4 * MEBI),
        name="distinct",
    )(cand_cat)
    wanted = exchange(wanted)
    by_event = history.transpose(1, 0, 2)
    rows = own_users * cand_count
    flat_cands = candidates.reshape(rows, width)
    span = math.lcm(16, own_users)
    far = pl.BlockSpec(memory_space=pltpu.HBM)
    stored, query, grouped = pl.pallas_call(
        lambda *refs: stage_kernel(*refs, own_users=own_users),
        out_shape=[
            pltpu.VMEM(by_event.shape, jnp.bfloat16),
            pltpu.VMEM((pairs, HEADS * cand_count, 2 * width), jnp.bfloat16),
            pltpu.VMEM((devices, block_events * span), jnp.float32),
        ],
        in_specs=[far] * 3,
        out_specs=[resident] * 3,
        scratch_shapes=[
            pltpu.VMEM((rows, width), jnp.bfloat16),
            pltpu.VMEM((block_events, users), jnp.int32),
            pltpu.SemaphoreType.DMA((2 + STREAMS,)),
        ],
        compiler_params=pltpu.CompilerParams(vmem_limit_bytes=24 * MEBI),
        name="stage",
    )(*[pltpu.with_memory_space_constraint(value, pltpu.HBM) for value in (by_event, flat_cands, event_cat.T)])
    packed = pl.pallas_call(
        lambda *refs: pack_kernel(*refs, own_users=own_users),
        out_shape=pltpu.VMEM((devices, (pairs + 1) * CAP, width), jnp.bfloat16),
        out_specs=resident,
        in_specs=[resident] * 3,
        compiler_params=pltpu.CompilerParams(vmem_limit_bytes=24 * MEBI),
        name="pack",
    )(near(wanted), near(grouped), near(stored))
    received = exchange(packed)
    slots = devices * CAP
    result = pl.pallas_call(
        tower_kernel,
        out_shape=jax.ShapeDtypeStruct((rows, width), jnp.bfloat16),
        in_specs=[resident] * 5,
        out_specs=pl.BlockSpec(memory_space=pltpu.HBM),
        scratch_shapes=[
            pltpu.VMEM((pairs, HEADS * cand_count, slots), jnp.float32),
            pltpu.VMEM((pairs, HEADS * cand_count, slots), jnp.bfloat16),
            pltpu.VMEM((pairs, HEADS * cand_count, 2 * width), jnp.float32),
            pltpu.VMEM((pairs, 2 * cand_count, width), jnp.float32),
            pltpu.VMEM((pairs, 2 * cand_count, w_input.shape[1]), jnp.float32),
            pltpu.VMEM((pairs, 2 * cand_count, w_input.shape[1]), jnp.bfloat16),
            pltpu.VMEM(w_input.shape, jnp.bfloat16),
            pltpu.VMEM((rows, width), jnp.bfloat16),
            pltpu.SemaphoreType.DMA((pairs,)),
        ],
        compiler_params=pltpu.CompilerParams(vmem_limit_bytes=40 * MEBI),
        name="tower",
    )(near(received), near(query), near(flat_cands), near(w_input), near(w_output))
    return result.reshape(own_users, cand_count, width)


def solution(mesh):
    placed = (
        P(None, AXES, None),
        P(None, AXES),
        P(AXES, None, None),
        P(AXES, None),
        P(),
        P(),
    )
    return jax.shard_map(
        local,
        mesh=mesh,
        in_specs=placed,
        out_specs=P(AXES, None, None),
        check_vma=False,
    )
```

```python
import math

import jax
import jax.numpy as jnp
from jax import lax
from jax.experimental import pallas as pl
from jax.experimental.pallas import tpu as pltpu
from jax.sharding import PartitionSpec as P

HEADS = 4
CAP = 8
QCAT = 8
LANES = 128
FINE = 8
HEAD_ORDER = (*range(0, HEADS, 2), *range(1, HEADS, 2))
BARRED = -1e30
MEBI = 1 << 20
STREAMS = 5
TILE = 2
AXES = ("role", "shard")


def iota(shape, dimension):
    return lax.broadcasted_iota(jnp.int32, shape, dimension)


def distinct_kernel(cat_ref, out_ref):
    cats = cat_ref[...].astype(jnp.float32)
    users = cats.shape[0]
    half = LANES // 2
    user = iota((users, LANES), 0)
    lane = iota((users, LANES), 1)
    beyond = jnp.float32(1e9)
    low = jnp.min(cats, axis=1, keepdims=True)
    high = jnp.max(cats, axis=1, keepdims=True)
    row = jnp.zeros((users, LANES), jnp.float32)
    for step in range(QCAT // 2):
        for place, value in ((step, low), (QCAT - 1 - step, high)):
            row = jnp.where(lane % half == place * users + user, value, row)
        if step + 1 < QCAT // 2:
            above = jnp.min(jnp.where(cats > low, cats, beyond), axis=1, keepdims=True)
            below = jnp.max(jnp.where(cats < high, cats, -beyond), axis=1, keepdims=True)
            low = jnp.where(above == beyond, low, above)
            high = jnp.where(below == -beyond, high, below)
    whole = jnp.sum(row, axis=0, keepdims=True).astype(jnp.int32)
    fine = whole & (FINE - 1)
    packed = jnp.where(iota((1, LANES), 1) < half, whole - fine, fine)
    out_ref[...] = jnp.broadcast_to(packed.reshape(1, 1, LANES), out_ref.shape)


def pack_kernel(wanted_ref, event_ref, history_ref, out_ref, *, own_users):
    devices = wanted_ref.shape[0]
    blocks_events = history_ref.shape[0]
    width = history_ref.shape[2]
    depth = event_ref.shape[1]
    span = depth // blocks_events
    per_group = span // own_users
    pairs = own_users // 2
    half = LANES // 2
    pad = -(-depth // LANES) * LANES
    wanted = wanted_ref[:, 0, :].astype(jnp.float32).astype(jnp.bfloat16)
    line = iota((LANES, pad), 0) % half
    mate = iota((LANES, pad), 1) % own_users
    events = event_ref[...]
    match = None
    for j in range(QCAT):
        spread = jnp.where(line == j * own_users + mate, 1.0, 0.0).astype(jnp.bfloat16)
        category = jnp.dot(wanted, spread, preferred_element_type=jnp.float32)[:, :depth]
        same = jnp.where(category == events, 1.0, 0.0)
        match = same if match is None else jnp.maximum(match, same)
    position = iota((devices, depth), 1) % span
    before = iota((depth, pad), 0)
    here = iota((depth, pad), 1)
    user_before = before % span
    user_here = here % span
    counted = (user_before == user_here) & (before <= here)
    counted = counted | ((user_here % 2 == 1) & (user_before == user_here - 1))
    counted = jnp.where(counted, 1.0, 0.0).astype(jnp.bfloat16)
    matched = match.astype(jnp.bfloat16)
    place = jnp.dot(matched, counted, preferred_element_type=jnp.float32)[:, :depth]
    pair_base = ((position % own_users) // 2 * CAP - 1).astype(jnp.float32)
    code = jnp.where(match > 0.0, place + pair_base, -1.0)
    lane = iota((depth, LANES), 1)
    leading = (lane < pairs) & (iota((depth, LANES), 0) % own_users == 2 * lane)
    leading = jnp.where(leading, 1.0, 0.0).astype(jnp.bfloat16)
    lead = jnp.dot(matched, leading, preferred_element_type=jnp.float32)
    rows = pairs * CAP
    row = iota((rows, depth), 0).astype(jnp.float32)
    for group in range(devices // per_group):
        stored = history_ref[:, group * span : (group + 1) * span, :].reshape(depth, width)
        picks = []
        for member in range(per_group):
            device = group * per_group + member
            picks.append(jnp.where(row == code[device : device + 1, :], 1.0, 0.0).astype(jnp.bfloat16))
        packed = jnp.dot(jnp.concatenate(picks, axis=0), stored, preferred_element_type=jnp.float32)
        for member in range(per_group):
            device = group * per_group + member
            block = packed[member * rows : (member + 1) * rows, :].astype(jnp.bfloat16)
            out_ref[device, : rows // TILE] = block.reshape(rows // TILE, TILE, width)
            out_ref[device, rows // TILE] = jnp.broadcast_to(lead[device : device + 1, :], (TILE, LANES)).astype(
                jnp.bfloat16
            )


def stage_kernel(
    history_ref, cand_ref, event_ref, stored_ref, query_ref, grouped_ref, cand_scratch, event_scratch, sems, *, own_users
):
    event_copy = pltpu.make_async_copy(event_ref, event_scratch, sems.at[0])
    cand_copy = pltpu.make_async_copy(cand_ref, cand_scratch, sems.at[1])
    events = history_ref.shape[0]
    cuts = [events * part // STREAMS for part in range(STREAMS + 1)]
    history_copies = [
        pltpu.make_async_copy(
            history_ref.at[pl.ds(low, high - low)], stored_ref.at[pl.ds(low, high - low)], sems.at[2 + part]
        )
        for part, (low, high) in enumerate(zip(cuts, cuts[1:]))
    ]
    event_copy.start()
    cand_copy.start()
    for copy in history_copies:
        copy.start()

    event_copy.wait()
    users = event_ref.shape[1]
    devices = users // own_users
    depth = grouped_ref.shape[1]
    span = depth // events
    fold = LANES // span
    owner = iota((devices, users), 1) // own_users == iota((devices, users), 0)
    parts = ([], [])
    for event in range(events):
        line = event_scratch[event : event + 1, :]
        fine = line & (FINE - 1)
        for part, value in zip(parts, (line - fine, fine)):
            part.append(jnp.where(owner, value.astype(jnp.float32), 0.0).astype(jnp.bfloat16))
    spread = jnp.where(iota((users, LANES), 0) % span == iota((users, LANES), 1) % span, 1.0, 0.0).astype(jnp.bfloat16)
    picked = sum(
        jnp.dot(jnp.concatenate(part, axis=0), spread, preferred_element_type=jnp.float32) for part in parts
    )
    lane = iota((devices, LANES), 1)
    mine = lane % span // own_users == iota((devices, LANES), 0) % (span // own_users)
    for first in range(0, events, fold):
        tile = jnp.full((devices, LANES), -1.0, jnp.float32)
        for event in range(first, min(first + fold, events)):
            rows = picked[event * devices : (event + 1) * devices, :]
            tile = jnp.where(mine & (lane // span == event - first), rows, tile)
        low = first * span
        high = min(low + LANES, depth)
        grouped_ref[:, low:high] = tile[:, : high - low]

    cand_copy.wait()
    width = cand_ref.shape[1]
    cand_count = query_ref.shape[1] // HEADS
    head_of = iota((cand_count, width), 1) // (width // HEADS)
    for pair in range(query_ref.shape[0]):
        for member in range(2):
            start = (2 * pair + member) * cand_count
            cands = cand_scratch[start : start + cand_count, :].astype(jnp.float32)
            heads = [jnp.where(head_of == head, cands, 0.0) for head in HEAD_ORDER]
            query_ref[pair, :, member * width : (member + 1) * width] = jnp.concatenate(heads, axis=0).astype(
                jnp.bfloat16
            )
    for copy in history_copies:
        copy.wait()


def chunks(total, most):
    best = total
    for size in range(8, most + 1, 8):
        if total % size == 0 and (size % 16 == 0 or total % 16):
            best = size
    return [(start, best) for start in range(0, total, best)]


def tower_kernel(
    packed_ref, query_ref, cand_ref, w_in_ref, w_out_ref, out_ref,
    score_ref, weight_ref, sum_ref, interest_ref, hidden_ref, active_ref, half_ref, result_ref, sems,
):
    pairs, head_rows, _ = query_ref.shape
    cand_count = head_rows // HEADS
    rows = 2 * cand_count
    width = cand_ref.shape[1]
    devices = packed_ref.shape[0]
    slots = devices * CAP
    head_size = width // HEADS
    scale = math.log2(math.e) * head_size ** (-0.5)
    lead = packed_ref[:, pairs * CAP // TILE].astype(jnp.float32)[:, :1, :]
    rank = iota((devices, CAP, LANES), 1).astype(jnp.float32)
    marks = jnp.where(rank < jnp.broadcast_to(lead, (devices, CAP, LANES)), 1.0, 0.0).reshape(slots, LANES)
    pick = jnp.where(iota((2 * CAP, LANES), 0) == iota((2 * CAP, LANES), 1), 1.0, 0.0).astype(jnp.bfloat16)
    across = lax.dot_general(
        pick, marks.astype(jnp.bfloat16), (((1,), (1,)), ((), ())), preferred_element_type=jnp.float32
    )
    slot_even = ((iota((slots, width), 1) // head_size) % 2).astype(jnp.float32).astype(jnp.bfloat16) == 0
    values = {}
    half_ref[...] = w_in_ref[...] * 0.5

    def score(pair):
        keys = packed_ref[:, pair * CAP // TILE : (pair + 1) * CAP // TILE]
        keys = keys.astype(jnp.float32).reshape(slots, width).astype(jnp.bfloat16)
        owned = jnp.broadcast_to(marks[:, pair : pair + 1], (slots, width)).astype(jnp.bfloat16)
        shared = 1 - owned
        own_keys = (keys * owned, keys * shared)
        right = jnp.concatenate(own_keys, axis=1)
        both = ((own_keys[0], owned), (own_keys[1], shared))
        values[pair] = (
            jnp.concatenate([jnp.where(slot_even, k, o) for k, o in both], axis=1),
            jnp.concatenate([jnp.where(slot_even, o, k) for k, o in both], axis=1),
        )
        score_ref[pair] = lax.dot_general(
            query_ref[pair], right, (((1,), (1,)), ((), ())), preferred_element_type=jnp.float32
        )

    def weigh(pair):
        mark = across[pair : pair + 1, :]
        bar_first = ((1.0 - mark) * BARRED).astype(jnp.bfloat16)
        bar_second = (mark * BARRED).astype(jnp.bfloat16)
        for start, size in chunks(head_rows, 160):
            scores = score_ref[pair, start : start + size, :]
            rough = scores.astype(jnp.bfloat16)
            peak_first = jnp.max(rough + bar_first, axis=1, keepdims=True).astype(jnp.float32)
            peak_second = jnp.max(rough + bar_second, axis=1, keepdims=True).astype(jnp.float32)
            peak = jnp.where(mark > 0.5, peak_first, peak_second)
            weight_ref[pair, start : start + size, :] = jnp.exp2((scores - peak) * scale).astype(jnp.bfloat16)

    def gather(pair):
        for block, head in enumerate(HEAD_ORDER):
            span = slice(block * cand_count, (block + 1) * cand_count)
            sum_ref[pair, span, :] = jnp.dot(
                weight_ref[pair, span, :], values[pair][head % 2], preferred_element_type=jnp.float32
            )

    def blend(pair):
        for start, size in chunks(cand_count, 40):
            head_of = iota((size, width), 1) // head_size
            for member in range(2):
                parts = [
                    sum_ref[
                        pair,
                        block * cand_count + start : block * cand_count + start + size,
                        member * width : (member + 1) * width,
                    ]
                    for block in map(HEAD_ORDER.index, range(HEADS))
                ]
                top = parts[0]
                total = parts[HEADS - 1]
                for head in range(1, HEADS):
                    top = jnp.where(head_of == head, parts[head], top)
                    total = jnp.where(head_of == head, parts[head - 1], total)
                inverse = pltpu.roll(1.0 / total, width - head_size, 1)
                interest_ref[pair, member * cand_count + start : member * cand_count + start + size, :] = (
                    top * inverse
                )

    def enter(pair):
        joined = jnp.concatenate(
            [cand_ref[pair * rows : (pair + 1) * rows, :], interest_ref[pair].astype(jnp.bfloat16)], axis=1
        )
        hidden_ref[pair] = jnp.dot(joined, half_ref[...], preferred_element_type=jnp.float32)

    def activate(pair):
        for start, size in chunks(rows, 16):
            middle = hidden_ref[pair, start : start + size, :]
            active_ref[pair, start : start + size, :] = (middle * jnp.tanh(middle) + middle).astype(jnp.bfloat16)

    def leave(pair):
        result = jnp.dot(active_ref[pair], w_out_ref[...], preferred_element_type=jnp.float32)
        result_ref[pair * rows : (pair + 1) * rows, :] = result.astype(jnp.bfloat16)
        copy_out(pair).start()

    def copy_out(pair):
        span = pl.ds(pair * rows, rows)
        return pltpu.make_async_copy(result_ref.at[span], out_ref.at[span], sems.at[pair])

    stages = (score, weigh, gather, blend, enter, activate, leave)
    begins = [pair // 2 * 5 for pair in range(pairs)]
    for tick in range(len(stages) + begins[-1]):
        for pair in range(pairs):
            stage = tick - begins[pair]
            if 0 <= stage < len(stages):
                stages[stage](pair)
    for pair in range(pairs):
        copy_out(pair).wait()


def near(value):
    return pltpu.with_memory_space_constraint(value, pltpu.VMEM)


def exchange(parts):
    return lax.all_to_all(parts, AXES, split_axis=0, concat_axis=0, tiled=True)


def local(history, event_cat, candidates, cand_cat, w_input, w_output):
    devices = lax.axis_size(AXES)
    own_users, cand_count, width = candidates.shape
    users, block_events = event_cat.shape
    pairs = own_users // 2
    resident = pl.BlockSpec(memory_space=pltpu.VMEM)
    wanted = pl.pallas_call(
        distinct_kernel,
        out_shape=pltpu.VMEM((devices, 1, LANES), jnp.int32),
        out_specs=resident,
        compiler_params=pltpu.CompilerParams(vmem_limit_bytes=4 * MEBI),
        name="distinct",
    )(cand_cat)
    wanted = exchange(wanted)
    by_event = history.transpose(1, 0, 2)
    rows = own_users * cand_count
    flat_cands = candidates.reshape(rows, width)
    span = math.lcm(16, own_users)
    far = pl.BlockSpec(memory_space=pltpu.HBM)
    stored, query, grouped = pl.pallas_call(
        lambda *refs: stage_kernel(*refs, own_users=own_users),
        out_shape=[
            pltpu.VMEM(by_event.shape, jnp.bfloat16),
            pltpu.VMEM((pairs, HEADS * cand_count, 2 * width), jnp.bfloat16),
            pltpu.VMEM((devices, block_events * span), jnp.float32),
        ],
        in_specs=[far] * 3,
        out_specs=[resident] * 3,
        scratch_shapes=[
            pltpu.VMEM((rows, width), jnp.bfloat16),
            pltpu.VMEM((block_events, users), jnp.int32),
            pltpu.SemaphoreType.DMA((2 + STREAMS,)),
        ],
        compiler_params=pltpu.CompilerParams(vmem_limit_bytes=24 * MEBI),
        name="stage",
    )(*[pltpu.with_memory_space_constraint(value, pltpu.HBM) for value in (by_event, flat_cands, event_cat.T)])
    packed = pl.pallas_call(
        lambda *refs: pack_kernel(*refs, own_users=own_users),
        out_shape=pltpu.VMEM((devices, pairs * CAP // TILE + 1, TILE, width), jnp.bfloat16),
        out_specs=resident,
        in_specs=[resident] * 3,
        compiler_params=pltpu.CompilerParams(vmem_limit_bytes=24 * MEBI),
        name="pack",
    )(near(wanted), near(grouped), near(stored))
    received = exchange(packed)
    slots = devices * CAP
    result = pl.pallas_call(
        tower_kernel,
        out_shape=jax.ShapeDtypeStruct((rows, width), jnp.bfloat16),
        in_specs=[resident] * 5,
        out_specs=pl.BlockSpec(memory_space=pltpu.HBM),
        scratch_shapes=[
            pltpu.VMEM((pairs, HEADS * cand_count, slots), jnp.float32),
            pltpu.VMEM((pairs, HEADS * cand_count, slots), jnp.bfloat16),
            pltpu.VMEM((pairs, HEADS * cand_count, 2 * width), jnp.float32),
            pltpu.VMEM((pairs, 2 * cand_count, width), jnp.float32),
            pltpu.VMEM((pairs, 2 * cand_count, w_input.shape[1]), jnp.float32),
            pltpu.VMEM((pairs, 2 * cand_count, w_input.shape[1]), jnp.bfloat16),
            pltpu.VMEM(w_input.shape, jnp.bfloat16),
            pltpu.VMEM((rows, width), jnp.bfloat16),
            pltpu.SemaphoreType.DMA((pairs,)),
        ],
        compiler_params=pltpu.CompilerParams(vmem_limit_bytes=40 * MEBI),
        name="tower",
    )(near(received), near(query), near(flat_cands), near(w_input), near(w_output))
    return result.reshape(own_users, cand_count, width)


def solution(mesh):
    placed = (
        P(None, AXES, None),
        P(None, AXES),
        P(AXES, None, None),
        P(AXES, None),
        P(),
        P(),
    )
    return jax.shard_map(
        local,
        mesh=mesh,
        in_specs=placed,
        out_specs=P(AXES, None, None),
        check_vma=False,
    )
```

```python
import math

import jax
import jax.numpy as jnp
from jax import lax
from jax.experimental import pallas as pl
from jax.experimental.pallas import tpu as pltpu
from jax.sharding import PartitionSpec as P

HEADS = 4
CAP = 8
QCAT = 8
LANES = 128
FINE = 8
HEAD_ORDER = (*range(0, HEADS, 2), *range(1, HEADS, 2))
BARRED = -1e30
MEBI = 1 << 20
STREAMS = 5
TILE = 2
AXES = ("role", "shard")


def iota(shape, dimension):
    return lax.broadcasted_iota(jnp.int32, shape, dimension)


def distinct_kernel(cat_ref, out_ref):
    cats = cat_ref[...].astype(jnp.float32)
    users = cats.shape[0]
    half = LANES // 2
    user = iota((users, LANES), 0)
    lane = iota((users, LANES), 1)
    beyond = jnp.float32(1e9)
    low = jnp.min(cats, axis=1, keepdims=True)
    high = jnp.max(cats, axis=1, keepdims=True)
    row = jnp.zeros((users, LANES), jnp.float32)
    for step in range(QCAT // 2):
        for place, value in ((step, low), (QCAT - 1 - step, high)):
            row = jnp.where(lane % half == place * users + user, value, row)
        if step + 1 < QCAT // 2:
            above = jnp.min(jnp.where(cats > low, cats, beyond), axis=1, keepdims=True)
            below = jnp.max(jnp.where(cats < high, cats, -beyond), axis=1, keepdims=True)
            low = jnp.where(above == beyond, low, above)
            high = jnp.where(below == -beyond, high, below)
    whole = jnp.sum(row, axis=0, keepdims=True).astype(jnp.int32)
    fine = whole & (FINE - 1)
    packed = jnp.where(iota((1, LANES), 1) < half, whole - fine, fine)
    out_ref[...] = jnp.broadcast_to(packed.reshape(1, 1, LANES), out_ref.shape)


def pack_kernel(wanted_ref, event_ref, history_ref, spread_ref, counted_ref, leading_ref, out_ref, *, own_users):
    devices = wanted_ref.shape[0]
    blocks_events = history_ref.shape[0]
    width = history_ref.shape[2]
    depth = event_ref.shape[1]
    span = depth // blocks_events
    per_group = span // own_users
    pairs = own_users // 2
    wanted = wanted_ref[:, 0, :].astype(jnp.float32).astype(jnp.bfloat16)
    events = event_ref[...]
    match = None
    for j in range(QCAT):
        category = jnp.dot(wanted, spread_ref[j], preferred_element_type=jnp.float32)[:, :depth]
        same = jnp.where(category == events, 1.0, 0.0)
        match = same if match is None else jnp.maximum(match, same)
    position = iota((devices, depth), 1) % span
    matched = match.astype(jnp.bfloat16)
    place = jnp.dot(matched, counted_ref[...], preferred_element_type=jnp.float32)[:, :depth]
    pair_base = ((position % own_users) // 2 * CAP - 1).astype(jnp.float32)
    code = jnp.where(match > 0.0, place + pair_base, -1.0)
    lead = jnp.dot(matched, leading_ref[...], preferred_element_type=jnp.float32)
    rows = pairs * CAP
    row = iota((rows, depth), 0).astype(jnp.float32).astype(jnp.bfloat16)
    for group in range(devices // per_group):
        stored = history_ref[:, group * span : (group + 1) * span, :].reshape(depth, width)
        picks = []
        for member in range(per_group):
            device = group * per_group + member
            own = jnp.broadcast_to(code[device : device + 1, :], row.shape).astype(jnp.bfloat16)
            picks.append(jnp.where(row == own, jnp.bfloat16(1), jnp.bfloat16(0)))
        packed = jnp.dot(jnp.concatenate(picks, axis=0), stored, preferred_element_type=jnp.float32)
        for member in range(per_group):
            device = group * per_group + member
            block = packed[member * rows : (member + 1) * rows, :].astype(jnp.bfloat16)
            out_ref[device, : rows // TILE] = block.reshape(rows // TILE, TILE, width)
            out_ref[device, rows // TILE] = jnp.broadcast_to(lead[device : device + 1, :], (TILE, LANES)).astype(
                jnp.bfloat16
            )


def stage_kernel(
    history_ref, cand_ref, event_ref,
    stored_ref, query_ref, grouped_ref, spread_ref, counted_ref, leading_ref,
    cand_scratch, event_scratch, sems, *, own_users,
):
    event_copy = pltpu.make_async_copy(event_ref, event_scratch, sems.at[0])
    cand_copy = pltpu.make_async_copy(cand_ref, cand_scratch, sems.at[1])
    events = history_ref.shape[0]
    cuts = [events * part // STREAMS for part in range(STREAMS + 1)]
    history_copies = [
        pltpu.make_async_copy(
            history_ref.at[pl.ds(low, high - low)], stored_ref.at[pl.ds(low, high - low)], sems.at[2 + part]
        )
        for part, (low, high) in enumerate(zip(cuts, cuts[1:]))
    ]
    event_copy.start()
    cand_copy.start()
    for copy in history_copies:
        copy.start()

    depth, pad = counted_ref.shape
    span = depth // events
    line = iota((LANES, pad), 0) % (LANES // 2)
    mate = iota((LANES, pad), 1) % own_users
    for j in range(QCAT):
        spread_ref[j] = jnp.where(line == j * own_users + mate, 1.0, 0.0).astype(jnp.bfloat16)
    before = iota((depth, pad), 0)
    here = iota((depth, pad), 1)
    user_before = before % span
    user_here = here % span
    counted = (user_before == user_here) & (before <= here)
    counted = counted | ((user_here % 2 == 1) & (user_before == user_here - 1))
    counted_ref[...] = jnp.where(counted, 1.0, 0.0).astype(jnp.bfloat16)
    lane = iota((depth, LANES), 1)
    leading = (lane < own_users // 2) & (iota((depth, LANES), 0) % own_users == 2 * lane)
    leading_ref[...] = jnp.where(leading, 1.0, 0.0).astype(jnp.bfloat16)

    event_copy.wait()
    users = event_ref.shape[1]
    devices = users // own_users
    fold = LANES // span
    owner = iota((devices, users), 1) // own_users == iota((devices, users), 0)
    parts = ([], [])
    for event in range(events):
        line = event_scratch[event : event + 1, :]
        fine = line & (FINE - 1)
        for part, value in zip(parts, (line - fine, fine)):
            part.append(jnp.where(owner, value.astype(jnp.float32), 0.0).astype(jnp.bfloat16))
    spread = jnp.where(iota((users, LANES), 0) % span == iota((users, LANES), 1) % span, 1.0, 0.0).astype(jnp.bfloat16)
    picked = sum(
        jnp.dot(jnp.concatenate(part, axis=0), spread, preferred_element_type=jnp.float32) for part in parts
    )
    lane = iota((devices, LANES), 1)
    mine = lane % span // own_users == iota((devices, LANES), 0) % (span // own_users)
    for first in range(0, events, fold):
        tile = jnp.full((devices, LANES), -1.0, jnp.float32)
        for event in range(first, min(first + fold, events)):
            rows = picked[event * devices : (event + 1) * devices, :]
            tile = jnp.where(mine & (lane // span == event - first), rows, tile)
        low = first * span
        high = min(low + LANES, depth)
        grouped_ref[:, low:high] = tile[:, : high - low]

    cand_copy.wait()
    width = cand_ref.shape[1]
    cand_count = query_ref.shape[1] // HEADS
    head_of = iota((cand_count, width), 1) // (width // HEADS)
    for pair in range(query_ref.shape[0]):
        for member in range(2):
            start = (2 * pair + member) * cand_count
            cands = cand_scratch[start : start + cand_count, :].astype(jnp.float32)
            heads = [jnp.where(head_of == head, cands, 0.0) for head in HEAD_ORDER]
            query_ref[pair, :, member * width : (member + 1) * width] = jnp.concatenate(heads, axis=0).astype(
                jnp.bfloat16
            )
    for copy in history_copies:
        copy.wait()


def chunks(total, most):
    best = total
    for size in range(8, most + 1, 8):
        if total % size == 0 and (size % 16 == 0 or total % 16):
            best = size
    return [(start, best) for start in range(0, total, best)]


def tower_kernel(
    packed_ref, query_ref, cand_ref, w_in_ref, w_out_ref, out_ref,
    score_ref, weight_ref, sum_ref, interest_ref, hidden_ref, active_ref, half_ref, result_ref, sems,
):
    pairs, head_rows, _ = query_ref.shape
    cand_count = head_rows // HEADS
    rows = 2 * cand_count
    width = cand_ref.shape[1]
    devices = packed_ref.shape[0]
    slots = devices * CAP
    head_size = width // HEADS
    scale = math.log2(math.e) * head_size ** (-0.5)
    lead = packed_ref[:, pairs * CAP // TILE].astype(jnp.float32)[:, :1, :]
    rank = iota((devices, CAP, LANES), 1).astype(jnp.float32)
    marks = jnp.where(rank < jnp.broadcast_to(lead, (devices, CAP, LANES)), 1.0, 0.0).reshape(slots, LANES)
    pick = jnp.where(iota((2 * CAP, LANES), 0) == iota((2 * CAP, LANES), 1), 1.0, 0.0).astype(jnp.bfloat16)
    across = lax.dot_general(
        pick, marks.astype(jnp.bfloat16), (((1,), (1,)), ((), ())), preferred_element_type=jnp.float32
    )
    slot_even = ((iota((slots, width), 1) // head_size) % 2).astype(jnp.float32).astype(jnp.bfloat16) == 0
    values = {}
    half_ref[...] = w_in_ref[...] * 0.5

    def score(pair):
        keys = packed_ref[:, pair * CAP // TILE : (pair + 1) * CAP // TILE]
        keys = keys.astype(jnp.float32).reshape(slots, width).astype(jnp.bfloat16)
        owned = jnp.broadcast_to(marks[:, pair : pair + 1], (slots, width)).astype(jnp.bfloat16)
        shared = 1 - owned
        own_keys = (keys * owned, keys * shared)
        right = jnp.concatenate(own_keys, axis=1)
        both = ((own_keys[0], owned), (own_keys[1], shared))
        values[pair] = (
            jnp.concatenate([jnp.where(slot_even, k, o) for k, o in both], axis=1),
            jnp.concatenate([jnp.where(slot_even, o, k) for k, o in both], axis=1),
        )
        score_ref[pair] = lax.dot_general(
            query_ref[pair], right, (((1,), (1,)), ((), ())), preferred_element_type=jnp.float32
        )

    def weigh(pair):
        mark = across[pair : pair + 1, :]
        bar_first = ((1.0 - mark) * BARRED).astype(jnp.bfloat16)
        bar_second = (mark * BARRED).astype(jnp.bfloat16)
        for start, size in chunks(head_rows, 160):
            scores = score_ref[pair, start : start + size, :]
            rough = scores.astype(jnp.bfloat16)
            peak_first = jnp.max(rough + bar_first, axis=1, keepdims=True).astype(jnp.float32)
            peak_second = jnp.max(rough + bar_second, axis=1, keepdims=True).astype(jnp.float32)
            peak = jnp.where(mark > 0.5, peak_first, peak_second)
            weight_ref[pair, start : start + size, :] = jnp.exp2((scores - peak) * scale).astype(jnp.bfloat16)

    def gather(pair):
        for parity in range(2):
            span = slice(parity * head_rows // 2, (parity + 1) * head_rows // 2)
            sum_ref[pair, span, :] = jnp.dot(
                weight_ref[pair, span, :], values[pair][parity], preferred_element_type=jnp.float32
            )

    def blend(pair):
        for start, size in chunks(cand_count, 40):
            head_of = iota((size, width), 1) // head_size
            for member in range(2):
                parts = [
                    sum_ref[
                        pair,
                        block * cand_count + start : block * cand_count + start + size,
                        member * width : (member + 1) * width,
                    ]
                    for block in map(HEAD_ORDER.index, range(HEADS))
                ]
                top = parts[0]
                total = parts[HEADS - 1]
                for head in range(1, HEADS):
                    top = jnp.where(head_of == head, parts[head], top)
                    total = jnp.where(head_of == head, parts[head - 1], total)
                inverse = pltpu.roll(1.0 / total, width - head_size, 1)
                interest_ref[pair, member * cand_count + start : member * cand_count + start + size, :] = (
                    top * inverse
                )

    def enter(pair):
        joined = jnp.concatenate(
            [cand_ref[pair * rows : (pair + 1) * rows, :], interest_ref[pair].astype(jnp.bfloat16)], axis=1
        )
        hidden_ref[pair] = jnp.dot(joined, half_ref[...], preferred_element_type=jnp.float32)

    def activate(pair):
        for start, size in chunks(rows, 16):
            middle = hidden_ref[pair, start : start + size, :]
            active_ref[pair, start : start + size, :] = (middle * jnp.tanh(middle) + middle).astype(jnp.bfloat16)

    def leave(pair):
        result = jnp.dot(active_ref[pair], w_out_ref[...], preferred_element_type=jnp.float32)
        result_ref[pair * rows : (pair + 1) * rows, :] = result.astype(jnp.bfloat16)
        copy_out(pair).start()

    def copy_out(pair):
        span = pl.ds(pair * rows, rows)
        return pltpu.make_async_copy(result_ref.at[span], out_ref.at[span], sems.at[pair])

    stages = (score, weigh, gather, blend, enter, activate, leave)
    begins = [pair // 2 * 5 + (pair % 2 if pair > 1 else 0) for pair in range(pairs)]
    for tick in range(len(stages) + begins[-1]):
        for pair in range(pairs):
            stage = tick - begins[pair]
            if 0 <= stage < len(stages):
                stages[stage](pair)
    for pair in range(pairs):
        copy_out(pair).wait()


def near(value):
    return pltpu.with_memory_space_constraint(value, pltpu.VMEM)


def exchange(parts):
    return lax.all_to_all(parts, AXES, split_axis=0, concat_axis=0, tiled=True)


def local(history, event_cat, candidates, cand_cat, w_input, w_output):
    devices = lax.axis_size(AXES)
    own_users, cand_count, width = candidates.shape
    users, block_events = event_cat.shape
    pairs = own_users // 2
    resident = pl.BlockSpec(memory_space=pltpu.VMEM)
    wanted = pl.pallas_call(
        distinct_kernel,
        out_shape=pltpu.VMEM((devices, 1, LANES), jnp.int32),
        out_specs=resident,
        compiler_params=pltpu.CompilerParams(vmem_limit_bytes=4 * MEBI),
        name="distinct",
    )(cand_cat)
    wanted = exchange(wanted)
    by_event = history.transpose(1, 0, 2)
    rows = own_users * cand_count
    flat_cands = candidates.reshape(rows, width)
    span = math.lcm(16, own_users)
    far = pl.BlockSpec(memory_space=pltpu.HBM)
    depth = block_events * span
    pad = -(-depth // LANES) * LANES
    stored, query, grouped, spread, counted, leading = pl.pallas_call(
        lambda *refs: stage_kernel(*refs, own_users=own_users),
        out_shape=[
            pltpu.VMEM(by_event.shape, jnp.bfloat16),
            pltpu.VMEM((pairs, HEADS * cand_count, 2 * width), jnp.bfloat16),
            pltpu.VMEM((devices, depth), jnp.float32),
            pltpu.VMEM((QCAT, LANES, pad), jnp.bfloat16),
            pltpu.VMEM((depth, pad), jnp.bfloat16),
            pltpu.VMEM((depth, LANES), jnp.bfloat16),
        ],
        in_specs=[far] * 3,
        out_specs=[resident] * 6,
        scratch_shapes=[
            pltpu.VMEM((rows, width), jnp.bfloat16),
            pltpu.VMEM((block_events, users), jnp.int32),
            pltpu.SemaphoreType.DMA((2 + STREAMS,)),
        ],
        compiler_params=pltpu.CompilerParams(vmem_limit_bytes=24 * MEBI),
        name="stage",
    )(*[pltpu.with_memory_space_constraint(value, pltpu.HBM) for value in (by_event, flat_cands, event_cat.T)])
    packed = pl.pallas_call(
        lambda *refs: pack_kernel(*refs, own_users=own_users),
        out_shape=pltpu.VMEM((devices, pairs * CAP // TILE + 1, TILE, width), jnp.bfloat16),
        out_specs=resident,
        in_specs=[resident] * 6,
        compiler_params=pltpu.CompilerParams(vmem_limit_bytes=24 * MEBI),
        name="pack",
    )(*[near(value) for value in (wanted, grouped, stored, spread, counted, leading)])
    received = exchange(packed)
    slots = devices * CAP
    result = pl.pallas_call(
        tower_kernel,
        out_shape=jax.ShapeDtypeStruct((rows, width), jnp.bfloat16),
        in_specs=[resident] * 5,
        out_specs=pl.BlockSpec(memory_space=pltpu.HBM),
        scratch_shapes=[
            pltpu.VMEM((pairs, HEADS * cand_count, slots), jnp.float32),
            pltpu.VMEM((pairs, HEADS * cand_count, slots), jnp.bfloat16),
            pltpu.VMEM((pairs, HEADS * cand_count, 2 * width), jnp.float32),
            pltpu.VMEM((pairs, 2 * cand_count, width), jnp.float32),
            pltpu.VMEM((pairs, 2 * cand_count, w_input.shape[1]), jnp.float32),
            pltpu.VMEM((pairs, 2 * cand_count, w_input.shape[1]), jnp.bfloat16),
            pltpu.VMEM(w_input.shape, jnp.bfloat16),
            pltpu.VMEM((rows, width), jnp.bfloat16),
            pltpu.SemaphoreType.DMA((pairs,)),
        ],
        compiler_params=pltpu.CompilerParams(vmem_limit_bytes=40 * MEBI),
        name="tower",
    )(near(received), near(query), near(flat_cands), near(w_input), near(w_output))
    return result.reshape(own_users, cand_count, width)


def solution(mesh):
    placed = (
        P(None, AXES, None),
        P(None, AXES),
        P(AXES, None, None),
        P(AXES, None),
        P(),
        P(),
    )
    return jax.shard_map(
        local,
        mesh=mesh,
        in_specs=placed,
        out_specs=P(AXES, None, None),
        check_vma=False,
    )
```

```python
import math

import jax
import jax.numpy as jnp
from jax import lax
from jax.experimental import pallas as pl
from jax.experimental.pallas import tpu as pltpu
from jax.sharding import PartitionSpec as P

HEADS = 4
CAP = 8
QCAT = 8
LANES = 128
FINE = 8
HEAD_ORDER = (*range(0, HEADS, 2), *range(1, HEADS, 2))
BARRED = -1e30
MEBI = 1 << 20
STREAMS = 5
TILE = 2
AXES = ("role", "shard")


def iota(shape, dimension):
    return lax.broadcasted_iota(jnp.int32, shape, dimension)


def distinct_kernel(cat_ref, out_ref):
    cats = cat_ref[...].astype(jnp.float32)
    users = cats.shape[0]
    half = LANES // 2
    user = iota((users, LANES), 0)
    lane = iota((users, LANES), 1)
    beyond = jnp.float32(1e9)
    low = jnp.min(cats, axis=1, keepdims=True)
    high = jnp.max(cats, axis=1, keepdims=True)
    row = jnp.zeros((users, LANES), jnp.float32)
    for step in range(QCAT // 2):
        for place, value in ((step, low), (QCAT - 1 - step, high)):
            row = jnp.where(lane % half == place * users + user, value, row)
        if step + 1 < QCAT // 2:
            above = jnp.min(jnp.where(cats > low, cats, beyond), axis=1, keepdims=True)
            below = jnp.max(jnp.where(cats < high, cats, -beyond), axis=1, keepdims=True)
            low = jnp.where(above == beyond, low, above)
            high = jnp.where(below == -beyond, high, below)
    whole = jnp.sum(row, axis=0, keepdims=True).astype(jnp.int32)
    fine = whole & (FINE - 1)
    packed = jnp.where(iota((1, LANES), 1) < half, whole - fine, fine)
    out_ref[...] = jnp.broadcast_to(packed.reshape(1, 1, LANES), out_ref.shape)


def pack_kernel(wanted_ref, event_ref, history_ref, out_ref, *, own_users):
    devices = wanted_ref.shape[0]
    blocks_events = history_ref.shape[0]
    width = history_ref.shape[2]
    depth = event_ref.shape[1]
    span = depth // blocks_events
    per_group = span // own_users
    pairs = own_users // 2
    half = LANES // 2
    pad = -(-depth // LANES) * LANES
    wanted = wanted_ref[:, 0, :].astype(jnp.float32).astype(jnp.bfloat16)
    line = iota((LANES, pad), 0) % half
    mate = iota((LANES, pad), 1) % own_users
    events = event_ref[...]
    match = None
    for j in range(QCAT):
        spread = jnp.where(line == j * own_users + mate, 1.0, 0.0).astype(jnp.bfloat16)
        category = jnp.dot(wanted, spread, preferred_element_type=jnp.float32)[:, :depth]
        same = jnp.where(category == events, 1.0, 0.0)
        match = same if match is None else jnp.maximum(match, same)
    position = iota((devices, depth), 1) % span
    before = iota((depth, pad), 0)
    here = iota((depth, pad), 1)
    user_before = before % span
    user_here = here % span
    counted = (user_before == user_here) & (before <= here)
    counted = counted | ((user_here % 2 == 1) & (user_before == user_here - 1))
    counted = jnp.where(counted, 1.0, 0.0).astype(jnp.bfloat16)
    matched = match.astype(jnp.bfloat16)
    place = jnp.dot(matched, counted, preferred_element_type=jnp.float32)[:, :depth]
    pair_base = ((position % own_users) // 2 * CAP - 1).astype(jnp.float32)
    code = jnp.where(match > 0.0, place + pair_base, -1.0)
    lane = iota((depth, LANES), 1)
    leading = (lane < pairs) & (iota((depth, LANES), 0) % own_users == 2 * lane)
    leading = jnp.where(leading, 1.0, 0.0).astype(jnp.bfloat16)
    lead = jnp.dot(matched, leading, preferred_element_type=jnp.float32)
    rows = pairs * CAP
    row = iota((rows, depth), 0).astype(jnp.float32)
    for group in range(devices // per_group):
        stored = history_ref[:, group * span : (group + 1) * span, :].reshape(depth, width)
        picks = []
        for member in range(per_group):
            device = group * per_group + member
            picks.append(jnp.where(row == code[device : device + 1, :], 1.0, 0.0).astype(jnp.bfloat16))
        packed = jnp.dot(jnp.concatenate(picks, axis=0), stored, preferred_element_type=jnp.float32)
        for member in range(per_group):
            device = group * per_group + member
            block = packed[member * rows : (member + 1) * rows, :].astype(jnp.bfloat16)
            out_ref[device, : rows // TILE] = block.reshape(rows // TILE, TILE, width)
            out_ref[device, rows // TILE] = jnp.broadcast_to(lead[device : device + 1, :], (TILE, LANES)).astype(
                jnp.bfloat16
            )


def stage_kernel(
    history_ref, cand_ref, event_ref, stored_ref, query_ref, grouped_ref, cand_scratch, event_scratch, sems, *, own_users
):
    event_copy = pltpu.make_async_copy(event_ref, event_scratch, sems.at[0])
    cand_copy = pltpu.make_async_copy(cand_ref, cand_scratch, sems.at[1])
    events = history_ref.shape[0]
    cuts = [events * part // STREAMS for part in range(STREAMS + 1)]
    history_copies = [
        pltpu.make_async_copy(
            history_ref.at[pl.ds(low, high - low)], stored_ref.at[pl.ds(low, high - low)], sems.at[2 + part]
        )
        for part, (low, high) in enumerate(zip(cuts, cuts[1:]))
    ]
    event_copy.start()
    cand_copy.start()
    for copy in history_copies:
        copy.start()

    event_copy.wait()
    users = event_ref.shape[1]
    devices = users // own_users
    depth = grouped_ref.shape[1]
    span = depth // events
    fold = LANES // span
    owner = iota((devices, users), 1) // own_users == iota((devices, users), 0)
    parts = ([], [])
    for event in range(events):
        line = event_scratch[event : event + 1, :]
        fine = line & (FINE - 1)
        for part, value in zip(parts, (line - fine, fine)):
            part.append(jnp.where(owner, value.astype(jnp.float32), 0.0).astype(jnp.bfloat16))
    spread = jnp.where(iota((users, LANES), 0) % span == iota((users, LANES), 1) % span, 1.0, 0.0).astype(jnp.bfloat16)
    picked = sum(
        jnp.dot(jnp.concatenate(part, axis=0), spread, preferred_element_type=jnp.float32) for part in parts
    )
    lane = iota((devices, LANES), 1)
    mine = lane % span // own_users == iota((devices, LANES), 0) % (span // own_users)
    for first in range(0, events, fold):
        tile = jnp.full((devices, LANES), -1.0, jnp.float32)
        for event in range(first, min(first + fold, events)):
            rows = picked[event * devices : (event + 1) * devices, :]
            tile = jnp.where(mine & (lane // span == event - first), rows, tile)
        low = first * span
        high = min(low + LANES, depth)
        grouped_ref[:, low:high] = tile[:, : high - low]

    cand_copy.wait()
    width = cand_ref.shape[1]
    cand_count = query_ref.shape[1] // HEADS
    head_of = iota((cand_count, width), 1) // (width // HEADS)
    for pair in range(query_ref.shape[0]):
        for member in range(2):
            start = (2 * pair + member) * cand_count
            cands = cand_scratch[start : start + cand_count, :].astype(jnp.float32)
            heads = [jnp.where(head_of == head, cands, 0.0) for head in HEAD_ORDER]
            query_ref[pair, :, member * width : (member + 1) * width] = jnp.concatenate(heads, axis=0).astype(
                jnp.bfloat16
            )
    for copy in history_copies:
        copy.wait()


def chunks(total, most):
    best = total
    for size in range(8, most + 1, 8):
        if total % size == 0 and (size % 16 == 0 or total % 16):
            best = size
    return [(start, best) for start in range(0, total, best)]


def tower_kernel(
    packed_ref, query_ref, cand_ref, w_in_ref, w_out_ref, out_ref,
    score_ref, weight_ref, sum_ref, interest_ref, hidden_ref, active_ref, half_ref, result_ref, sems,
):
    pairs, head_rows, _ = query_ref.shape
    cand_count = head_rows // HEADS
    rows = 2 * cand_count
    width = cand_ref.shape[1]
    devices = packed_ref.shape[0]
    slots = devices * CAP
    head_size = width // HEADS
    scale = math.log2(math.e) * head_size ** (-0.5)
    lead = packed_ref[:, pairs * CAP // TILE].astype(jnp.float32)[:, :1, :]
    rank = iota((devices, CAP, LANES), 1).astype(jnp.float32)
    marks = jnp.where(rank < jnp.broadcast_to(lead, (devices, CAP, LANES)), 1.0, 0.0).reshape(slots, LANES)
    pick = jnp.where(iota((2 * CAP, LANES), 0) == iota((2 * CAP, LANES), 1), 1.0, 0.0).astype(jnp.bfloat16)
    across = lax.dot_general(
        pick, marks.astype(jnp.bfloat16), (((1,), (1,)), ((), ())), preferred_element_type=jnp.float32
    )
    slot_even = ((iota((slots, width), 1) // head_size) % 2).astype(jnp.float32).astype(jnp.bfloat16) == 0
    values = {}
    half_ref[...] = w_in_ref[...] * 0.5

    def score(pair):
        keys = packed_ref[:, pair * CAP // TILE : (pair + 1) * CAP // TILE]
        keys = keys.astype(jnp.float32).reshape(slots, width).astype(jnp.bfloat16)
        owned = jnp.broadcast_to(marks[:, pair : pair + 1], (slots, width)).astype(jnp.bfloat16)
        shared = 1 - owned
        own_keys = (keys * owned, keys * shared)
        right = jnp.concatenate(own_keys, axis=1)
        both = ((own_keys[0], owned), (own_keys[1], shared))
        values[pair] = (
            jnp.concatenate([jnp.where(slot_even, k, o) for k, o in both], axis=1),
            jnp.concatenate([jnp.where(slot_even, o, k) for k, o in both], axis=1),
        )
        score_ref[pair] = lax.dot_general(
            query_ref[pair], right, (((1,), (1,)), ((), ())), preferred_element_type=jnp.float32
        )

    def weigh(pair):
        mark = across[pair : pair + 1, :]
        bar_first = ((1.0 - mark) * BARRED).astype(jnp.bfloat16)
        bar_second = (mark * BARRED).astype(jnp.bfloat16)
        for start, size in chunks(head_rows, 160):
            scores = score_ref[pair, start : start + size, :]
            rough = scores.astype(jnp.bfloat16)
            peak_first = jnp.max(rough + bar_first, axis=1, keepdims=True).astype(jnp.float32)
            peak_second = jnp.max(rough + bar_second, axis=1, keepdims=True).astype(jnp.float32)
            peak = jnp.where(mark > 0.5, peak_first, peak_second)
            weight_ref[pair, start : start + size, :] = jnp.exp2((scores - peak) * scale).astype(jnp.bfloat16)

    def gather(pair):
        for parity in range(2):
            span = slice(parity * head_rows // 2, (parity + 1) * head_rows // 2)
            sum_ref[pair, span, :] = jnp.dot(
                weight_ref[pair, span, :], values[pair][parity], preferred_element_type=jnp.float32
            )

    def blend(pair):
        for start, size in chunks(cand_count, 40):
            head_of = iota((size, width), 1) // head_size
            for member in range(2):
                parts = [
                    sum_ref[
                        pair,
                        block * cand_count + start : block * cand_count + start + size,
                        member * width : (member + 1) * width,
                    ]
                    for block in map(HEAD_ORDER.index, range(HEADS))
                ]
                top = parts[0]
                total = parts[HEADS - 1]
                for head in range(1, HEADS):
                    top = jnp.where(head_of == head, parts[head], top)
                    total = jnp.where(head_of == head, parts[head - 1], total)
                inverse = pltpu.roll(1.0 / total, width - head_size, 1)
                interest_ref[pair, member * cand_count + start : member * cand_count + start + size, :] = (
                    top * inverse
                )

    def enter(pair):
        joined = jnp.concatenate(
            [cand_ref[pair * rows : (pair + 1) * rows, :], interest_ref[pair].astype(jnp.bfloat16)], axis=1
        )
        hidden_ref[pair] = jnp.dot(joined, half_ref[...], preferred_element_type=jnp.float32)

    def activate(pair):
        for start, size in chunks(rows, 16):
            middle = hidden_ref[pair, start : start + size, :]
            active_ref[pair, start : start + size, :] = (middle * jnp.tanh(middle) + middle).astype(jnp.bfloat16)

    def leave(pair):
        result = jnp.dot(active_ref[pair], w_out_ref[...], preferred_element_type=jnp.float32)
        result_ref[pair * rows : (pair + 1) * rows, :] = result.astype(jnp.bfloat16)
        copy_out(pair).start()

    def copy_out(pair):
        span = pl.ds(pair * rows, rows)
        return pltpu.make_async_copy(result_ref.at[span], out_ref.at[span], sems.at[pair])

    stages = (score, weigh, gather, blend, enter, activate, leave)
    begins = [pair // 2 * 5 + (pair % 2 if pair > 1 else 0) for pair in range(pairs)]
    for tick in range(len(stages) + begins[-1]):
        for pair in range(pairs):
            stage = tick - begins[pair]
            if 0 <= stage < len(stages):
                stages[stage](pair)
    for pair in range(pairs):
        copy_out(pair).wait()


def near(value):
    return pltpu.with_memory_space_constraint(value, pltpu.VMEM)


def exchange(parts):
    return lax.all_to_all(parts, AXES, split_axis=0, concat_axis=0, tiled=True)


def local(history, event_cat, candidates, cand_cat, w_input, w_output):
    devices = lax.axis_size(AXES)
    own_users, cand_count, width = candidates.shape
    users, block_events = event_cat.shape
    pairs = own_users // 2
    resident = pl.BlockSpec(memory_space=pltpu.VMEM)
    wanted = pl.pallas_call(
        distinct_kernel,
        out_shape=pltpu.VMEM((devices, 1, LANES), jnp.int32),
        out_specs=resident,
        compiler_params=pltpu.CompilerParams(vmem_limit_bytes=4 * MEBI),
        name="distinct",
    )(cand_cat)
    wanted = exchange(wanted)
    by_event = history.transpose(1, 0, 2)
    rows = own_users * cand_count
    flat_cands = candidates.reshape(rows, width)
    span = math.lcm(16, own_users)
    far = pl.BlockSpec(memory_space=pltpu.HBM)
    stored, query, grouped = pl.pallas_call(
        lambda *refs: stage_kernel(*refs, own_users=own_users),
        out_shape=[
            pltpu.VMEM(by_event.shape, jnp.bfloat16),
            pltpu.VMEM((pairs, HEADS * cand_count, 2 * width), jnp.bfloat16),
            pltpu.VMEM((devices, block_events * span), jnp.float32),
        ],
        in_specs=[far] * 3,
        out_specs=[resident] * 3,
        scratch_shapes=[
            pltpu.VMEM((rows, width), jnp.bfloat16),
            pltpu.VMEM((block_events, users), jnp.int32),
            pltpu.SemaphoreType.DMA((2 + STREAMS,)),
        ],
        compiler_params=pltpu.CompilerParams(vmem_limit_bytes=24 * MEBI),
        name="stage",
    )(*[pltpu.with_memory_space_constraint(value, pltpu.HBM) for value in (by_event, flat_cands, event_cat.T)])
    packed = pl.pallas_call(
        lambda *refs: pack_kernel(*refs, own_users=own_users),
        out_shape=pltpu.VMEM((devices, pairs * CAP // TILE + 1, TILE, width), jnp.bfloat16),
        out_specs=resident,
        in_specs=[resident] * 3,
        compiler_params=pltpu.CompilerParams(vmem_limit_bytes=24 * MEBI),
        name="pack",
    )(near(wanted), near(grouped), near(stored))
    received = exchange(packed)
    slots = devices * CAP
    result = pl.pallas_call(
        tower_kernel,
        out_shape=jax.ShapeDtypeStruct((rows, width), jnp.bfloat16),
        in_specs=[resident] * 5,
        out_specs=pl.BlockSpec(memory_space=pltpu.HBM),
        scratch_shapes=[
            pltpu.VMEM((pairs, HEADS * cand_count, slots), jnp.float32),
            pltpu.VMEM((pairs, HEADS * cand_count, slots), jnp.bfloat16),
            pltpu.VMEM((pairs, HEADS * cand_count, 2 * width), jnp.float32),
            pltpu.VMEM((pairs, 2 * cand_count, width), jnp.float32),
            pltpu.VMEM((pairs, 2 * cand_count, w_input.shape[1]), jnp.float32),
            pltpu.VMEM((pairs, 2 * cand_count, w_input.shape[1]), jnp.bfloat16),
            pltpu.VMEM(w_input.shape, jnp.bfloat16),
            pltpu.VMEM((rows, width), jnp.bfloat16),
            pltpu.SemaphoreType.DMA((pairs,)),
        ],
        compiler_params=pltpu.CompilerParams(vmem_limit_bytes=40 * MEBI),
        name="tower",
    )(near(received), near(query), near(flat_cands), near(w_input), near(w_output))
    return result.reshape(own_users, cand_count, width)


def solution(mesh):
    placed = (
        P(None, AXES, None),
        P(None, AXES),
        P(AXES, None, None),
        P(AXES, None),
        P(),
        P(),
    )
    return jax.shard_map(
        local,
        mesh=mesh,
        in_specs=placed,
        out_specs=P(AXES, None, None),
        check_vma=False,
    )
```

```python
import math

import jax
import jax.numpy as jnp
from jax import lax
from jax.experimental import pallas as pl
from jax.experimental.pallas import tpu as pltpu
from jax.sharding import PartitionSpec as P

HEADS = 4
CAP = 8
QCAT = 8
LANES = 128
FINE = 8
HEAD_ORDER = (*range(0, HEADS, 2), *range(1, HEADS, 2))
BARRED = -1e30
MEBI = 1 << 20
STREAMS = 5
TILE = 2
AXES = ("role", "shard")


def iota(shape, dimension):
    return lax.broadcasted_iota(jnp.int32, shape, dimension)


def distinct_kernel(cat_ref, out_ref):
    cats = cat_ref[...].astype(jnp.float32)
    users = cats.shape[0]
    half = LANES // 2
    user = iota((users, LANES), 0)
    lane = iota((users, LANES), 1)
    beyond = jnp.float32(1e9)
    low = jnp.min(cats, axis=1, keepdims=True)
    high = jnp.max(cats, axis=1, keepdims=True)
    row = jnp.zeros((users, LANES), jnp.float32)
    for step in range(QCAT // 2):
        for place, value in ((step, low), (QCAT - 1 - step, high)):
            row = jnp.where(lane % half == place * users + user, value, row)
        if step + 1 < QCAT // 2:
            above = jnp.min(jnp.where(cats > low, cats, beyond), axis=1, keepdims=True)
            below = jnp.max(jnp.where(cats < high, cats, -beyond), axis=1, keepdims=True)
            low = jnp.where(above == beyond, low, above)
            high = jnp.where(below == -beyond, high, below)
    whole = jnp.sum(row, axis=0, keepdims=True).astype(jnp.int32)
    fine = whole & (FINE - 1)
    packed = jnp.where(iota((1, LANES), 1) < half, whole - fine, fine)
    out_ref[...] = jnp.broadcast_to(packed.reshape(1, 1, LANES), out_ref.shape)


def pack_kernel(wanted_ref, event_ref, history_ref, out_ref, *, own_users):
    devices = wanted_ref.shape[0]
    blocks_events = history_ref.shape[0]
    width = history_ref.shape[2]
    depth = event_ref.shape[1]
    span = depth // blocks_events
    per_group = span // own_users
    pairs = own_users // 2
    half = LANES // 2
    pad = -(-depth // LANES) * LANES
    wanted = wanted_ref[:, 0, :].astype(jnp.float32).astype(jnp.bfloat16)
    line = iota((LANES, pad), 0) % half
    mate = iota((LANES, pad), 1) % own_users
    events = event_ref[...]
    match = None
    for j in range(QCAT):
        spread = jnp.where(line == j * own_users + mate, 1.0, 0.0).astype(jnp.bfloat16)
        category = jnp.dot(wanted, spread, preferred_element_type=jnp.float32)[:, :depth]
        same = jnp.where(category == events, 1.0, 0.0)
        match = same if match is None else jnp.maximum(match, same)
    position = iota((devices, depth), 1) % span
    before = iota((depth, pad), 0)
    here = iota((depth, pad), 1)
    user_before = before % span
    user_here = here % span
    counted = (user_before == user_here) & (before <= here)
    counted = counted | ((user_here % 2 == 1) & (user_before == user_here - 1))
    counted = jnp.where(counted, 1.0, 0.0).astype(jnp.bfloat16)
    matched = match.astype(jnp.bfloat16)
    place = jnp.dot(matched, counted, preferred_element_type=jnp.float32)[:, :depth]
    pair_base = ((position % own_users) // 2 * CAP - 1).astype(jnp.float32)
    code = jnp.where(match > 0.0, place + pair_base, -1.0)
    lane = iota((depth, LANES), 1)
    leading = (lane < pairs) & (iota((depth, LANES), 0) % own_users == 2 * lane)
    leading = jnp.where(leading, 1.0, 0.0).astype(jnp.bfloat16)
    lead = jnp.dot(matched, leading, preferred_element_type=jnp.float32)
    rows = pairs * CAP
    row = iota((rows, depth), 0).astype(jnp.float32)
    for group in range(devices // per_group):
        stored = history_ref[:, group * span : (group + 1) * span, :].reshape(depth, width)
        picks = []
        for member in range(per_group):
            device = group * per_group + member
            picks.append(jnp.where(row == code[device : device + 1, :], 1.0, 0.0).astype(jnp.bfloat16))
        packed = jnp.dot(jnp.concatenate(picks, axis=0), stored, preferred_element_type=jnp.float32)
        for member in range(per_group):
            device = group * per_group + member
            block = packed[member * rows : (member + 1) * rows, :].astype(jnp.bfloat16)
            out_ref[device, : rows // TILE] = block.reshape(rows // TILE, TILE, width)
            out_ref[device, rows // TILE] = jnp.broadcast_to(lead[device : device + 1, :], (TILE, LANES)).astype(
                jnp.bfloat16
            )


def stage_kernel(
    history_ref, cand_ref, event_ref, stored_ref, query_ref, grouped_ref, cand_scratch, event_scratch, sems, *, own_users
):
    event_copy = pltpu.make_async_copy(event_ref, event_scratch, sems.at[0])
    cand_copy = pltpu.make_async_copy(cand_ref, cand_scratch, sems.at[1])
    events = history_ref.shape[0]
    cuts = [events * part // STREAMS for part in range(STREAMS + 1)]
    history_copies = [
        pltpu.make_async_copy(
            history_ref.at[pl.ds(low, high - low)], stored_ref.at[pl.ds(low, high - low)], sems.at[2 + part]
        )
        for part, (low, high) in enumerate(zip(cuts, cuts[1:]))
    ]
    event_copy.start()
    cand_copy.start()
    for copy in history_copies:
        copy.start()

    event_copy.wait()
    users = event_ref.shape[1]
    devices = users // own_users
    depth = grouped_ref.shape[1]
    span = depth // events
    fold = LANES // span
    owner = iota((devices, users), 1) // own_users == iota((devices, users), 0)
    parts = ([], [])
    for event in range(events):
        line = event_scratch[event : event + 1, :]
        fine = line & (FINE - 1)
        for part, value in zip(parts, (line - fine, fine)):
            part.append(jnp.where(owner, value.astype(jnp.float32), 0.0).astype(jnp.bfloat16))
    spread = jnp.where(iota((users, LANES), 0) % span == iota((users, LANES), 1) % span, 1.0, 0.0).astype(jnp.bfloat16)
    picked = sum(
        jnp.dot(jnp.concatenate(part, axis=0), spread, preferred_element_type=jnp.float32) for part in parts
    )
    lane = iota((devices, LANES), 1)
    mine = lane % span // own_users == iota((devices, LANES), 0) % (span // own_users)
    for first in range(0, events, fold):
        tile = jnp.full((devices, LANES), -1.0, jnp.float32)
        for event in range(first, min(first + fold, events)):
            rows = picked[event * devices : (event + 1) * devices, :]
            tile = jnp.where(mine & (lane // span == event - first), rows, tile)
        low = first * span
        high = min(low + LANES, depth)
        grouped_ref[:, low:high] = tile[:, : high - low]

    cand_copy.wait()
    width = cand_ref.shape[1]
    cand_count = query_ref.shape[1] // HEADS
    head_of = iota((cand_count, width), 1) // (width // HEADS)
    for pair in range(query_ref.shape[0]):
        for member in range(2):
            start = (2 * pair + member) * cand_count
            cands = cand_scratch[start : start + cand_count, :].astype(jnp.float32)
            heads = [jnp.where(head_of == head, cands, 0.0) for head in HEAD_ORDER]
            query_ref[pair, :, member * width : (member + 1) * width] = jnp.concatenate(heads, axis=0).astype(
                jnp.bfloat16
            )
    for copy in history_copies:
        copy.wait()


def chunks(total, most):
    best = total
    for size in range(8, most + 1, 8):
        if total % size == 0 and (size % 16 == 0 or total % 16):
            best = size
    return [(start, best) for start in range(0, total, best)]


def tower_kernel(
    packed_ref, query_ref, cand_ref, w_in_ref, w_out_ref, out_ref,
    score_ref, weight_ref, sum_ref, interest_ref, hidden_ref, active_ref, half_ref, result_ref, sems,
):
    pairs, head_rows, _ = query_ref.shape
    cand_count = head_rows // HEADS
    rows = 2 * cand_count
    width = cand_ref.shape[1]
    devices = packed_ref.shape[0]
    slots = devices * CAP
    head_size = width // HEADS
    scale = math.log2(math.e) * head_size ** (-0.5)
    lead = packed_ref[:, pairs * CAP // TILE].astype(jnp.float32)[:, :1, :]
    rank = iota((devices, CAP, LANES), 1).astype(jnp.float32)
    marks = jnp.where(rank < jnp.broadcast_to(lead, (devices, CAP, LANES)), 1.0, 0.0).reshape(slots, LANES)
    pick = jnp.where(iota((2 * CAP, LANES), 0) == iota((2 * CAP, LANES), 1), 1.0, 0.0).astype(jnp.bfloat16)
    across = lax.dot_general(
        pick, marks.astype(jnp.bfloat16), (((1,), (1,)), ((), ())), preferred_element_type=jnp.float32
    )
    slot_even = ((iota((slots, width), 1) // head_size) % 2).astype(jnp.float32).astype(jnp.bfloat16) == 0
    values = {}
    half_ref[...] = w_in_ref[...] * 0.5

    def score(pair):
        keys = packed_ref[:, pair * CAP // TILE : (pair + 1) * CAP // TILE]
        keys = keys.astype(jnp.float32).reshape(slots, width).astype(jnp.bfloat16)
        owned = jnp.broadcast_to(marks[:, pair : pair + 1], (slots, width)).astype(jnp.bfloat16)
        shared = 1 - owned
        own_keys = (keys * owned, keys * shared)
        right = jnp.concatenate(own_keys, axis=1)
        both = ((own_keys[0], owned), (own_keys[1], shared))
        values[pair] = (
            jnp.concatenate([jnp.where(slot_even, k, o) for k, o in both], axis=1),
            jnp.concatenate([jnp.where(slot_even, o, k) for k, o in both], axis=1),
        )
        score_ref[pair] = lax.dot_general(
            query_ref[pair], right, (((1,), (1,)), ((), ())), preferred_element_type=jnp.float32
        )

    def weigh(pair):
        mark = across[pair : pair + 1, :]
        firsts = mark.astype(jnp.bfloat16) > 0.5
        bar_first = ((1.0 - mark) * BARRED).astype(jnp.bfloat16)
        bar_second = (mark * BARRED).astype(jnp.bfloat16)
        for start, size in chunks(head_rows, 160):
            scores = score_ref[pair, start : start + size, :]
            rough = scores.astype(jnp.bfloat16)
            peak_first = jnp.max(rough + bar_first, axis=1, keepdims=True)
            peak_second = jnp.max(rough + bar_second, axis=1, keepdims=True)
            peak = jnp.where(firsts, peak_first, peak_second).astype(jnp.float32)
            weight_ref[pair, start : start + size, :] = jnp.exp2((scores - peak) * scale).astype(jnp.bfloat16)

    def gather(pair):
        for parity in range(2):
            span = slice(parity * head_rows // 2, (parity + 1) * head_rows // 2)
            sum_ref[pair, span, :] = jnp.dot(
                weight_ref[pair, span, :], values[pair][parity], preferred_element_type=jnp.float32
            )

    def blend(pair):
        for start, size in chunks(cand_count, 40):
            head_of = iota((size, width), 1) // head_size
            for member in range(2):
                parts = [
                    sum_ref[
                        pair,
                        block * cand_count + start : block * cand_count + start + size,
                        member * width : (member + 1) * width,
                    ]
                    for block in map(HEAD_ORDER.index, range(HEADS))
                ]
                top = parts[0]
                total = parts[HEADS - 1]
                for head in range(1, HEADS):
                    top = jnp.where(head_of == head, parts[head], top)
                    total = jnp.where(head_of == head, parts[head - 1], total)
                inverse = pltpu.roll(1.0 / total, width - head_size, 1)
                interest_ref[pair, member * cand_count + start : member * cand_count + start + size, :] = (
                    top * inverse
                )

    def enter(pair):
        joined = jnp.concatenate(
            [cand_ref[pair * rows : (pair + 1) * rows, :], interest_ref[pair].astype(jnp.bfloat16)], axis=1
        )
        hidden_ref[pair] = jnp.dot(joined, half_ref[...], preferred_element_type=jnp.float32)

    def activate(pair):
        for start, size in chunks(rows, 16):
            middle = hidden_ref[pair, start : start + size, :]
            active_ref[pair, start : start + size, :] = (middle * jnp.tanh(middle) + middle).astype(jnp.bfloat16)

    def leave(pair):
        result = jnp.dot(active_ref[pair], w_out_ref[...], preferred_element_type=jnp.float32)
        result_ref[pair * rows : (pair + 1) * rows, :] = result.astype(jnp.bfloat16)
        copy_out(pair).start()

    def copy_out(pair):
        span = pl.ds(pair * rows, rows)
        return pltpu.make_async_copy(result_ref.at[span], out_ref.at[span], sems.at[pair])

    stages = (score, weigh, gather, blend, enter, activate, leave)
    begins = [pair // 2 * 5 + (pair % 2 if pair > 1 else 0) for pair in range(pairs)]
    for tick in range(len(stages) + begins[-1]):
        for pair in range(pairs):
            stage = tick - begins[pair]
            if 0 <= stage < len(stages):
                stages[stage](pair)
    for pair in range(pairs):
        copy_out(pair).wait()


def near(value):
    return pltpu.with_memory_space_constraint(value, pltpu.VMEM)


def exchange(parts):
    return lax.all_to_all(parts, AXES, split_axis=0, concat_axis=0, tiled=True)


def local(history, event_cat, candidates, cand_cat, w_input, w_output):
    devices = lax.axis_size(AXES)
    own_users, cand_count, width = candidates.shape
    users, block_events = event_cat.shape
    pairs = own_users // 2
    resident = pl.BlockSpec(memory_space=pltpu.VMEM)
    wanted = pl.pallas_call(
        distinct_kernel,
        out_shape=pltpu.VMEM((devices, 1, LANES), jnp.int32),
        out_specs=resident,
        compiler_params=pltpu.CompilerParams(vmem_limit_bytes=4 * MEBI),
        name="distinct",
    )(cand_cat)
    wanted = exchange(wanted)
    by_event = history.transpose(1, 0, 2)
    rows = own_users * cand_count
    flat_cands = candidates.reshape(rows, width)
    span = math.lcm(16, own_users)
    far = pl.BlockSpec(memory_space=pltpu.HBM)
    stored, query, grouped = pl.pallas_call(
        lambda *refs: stage_kernel(*refs, own_users=own_users),
        out_shape=[
            pltpu.VMEM(by_event.shape, jnp.bfloat16),
            pltpu.VMEM((pairs, HEADS * cand_count, 2 * width), jnp.bfloat16),
            pltpu.VMEM((devices, block_events * span), jnp.float32),
        ],
        in_specs=[far] * 3,
        out_specs=[resident] * 3,
        scratch_shapes=[
            pltpu.VMEM((rows, width), jnp.bfloat16),
            pltpu.VMEM((block_events, users), jnp.int32),
            pltpu.SemaphoreType.DMA((2 + STREAMS,)),
        ],
        compiler_params=pltpu.CompilerParams(vmem_limit_bytes=24 * MEBI),
        name="stage",
    )(*[pltpu.with_memory_space_constraint(value, pltpu.HBM) for value in (by_event, flat_cands, event_cat.T)])
    packed = pl.pallas_call(
        lambda *refs: pack_kernel(*refs, own_users=own_users),
        out_shape=pltpu.VMEM((devices, pairs * CAP // TILE + 1, TILE, width), jnp.bfloat16),
        out_specs=resident,
        in_specs=[resident] * 3,
        compiler_params=pltpu.CompilerParams(vmem_limit_bytes=24 * MEBI),
        name="pack",
    )(near(wanted), near(grouped), near(stored))
    received = exchange(packed)
    slots = devices * CAP
    result = pl.pallas_call(
        tower_kernel,
        out_shape=jax.ShapeDtypeStruct((rows, width), jnp.bfloat16),
        in_specs=[resident] * 5,
        out_specs=pl.BlockSpec(memory_space=pltpu.HBM),
        scratch_shapes=[
            pltpu.VMEM((pairs, HEADS * cand_count, slots), jnp.float32),
            pltpu.VMEM((pairs, HEADS * cand_count, slots), jnp.bfloat16),
            pltpu.VMEM((pairs, HEADS * cand_count, 2 * width), jnp.float32),
            pltpu.VMEM((pairs, 2 * cand_count, width), jnp.float32),
            pltpu.VMEM((pairs, 2 * cand_count, w_input.shape[1]), jnp.float32),
            pltpu.VMEM((pairs, 2 * cand_count, w_input.shape[1]), jnp.bfloat16),
            pltpu.VMEM(w_input.shape, jnp.bfloat16),
            pltpu.VMEM((rows, width), jnp.bfloat16),
            pltpu.SemaphoreType.DMA((pairs,)),
        ],
        compiler_params=pltpu.CompilerParams(vmem_limit_bytes=40 * MEBI),
        name="tower",
    )(near(received), near(query), near(flat_cands), near(w_input), near(w_output))
    return result.reshape(own_users, cand_count, width)


def solution(mesh):
    placed = (
        P(None, AXES, None),
        P(None, AXES),
        P(AXES, None, None),
        P(AXES, None),
        P(),
        P(),
    )
    return jax.shard_map(
        local,
        mesh=mesh,
        in_specs=placed,
        out_specs=P(AXES, None, None),
        check_vma=False,
    )
```

```python
import math

import jax
import jax.numpy as jnp
from jax import lax
from jax.experimental import pallas as pl
from jax.experimental.pallas import tpu as pltpu
from jax.sharding import PartitionSpec as P

HEADS = 4
CAP = 8
QCAT = 8
LANES = 128
FINE = 8
HEAD_ORDER = (*range(0, HEADS, 2), *range(1, HEADS, 2))
BARRED = -1e30
MEBI = 1 << 20
STREAMS = 5
TILE = 2
AXES = ("role", "shard")


def iota(shape, dimension):
    return lax.broadcasted_iota(jnp.int32, shape, dimension)


def distinct_kernel(cat_ref, out_ref):
    cats = cat_ref[...].astype(jnp.float32)
    users = cats.shape[0]
    half = LANES // 2
    user = iota((users, LANES), 0)
    lane = iota((users, LANES), 1)
    beyond = jnp.float32(1e9)
    low = jnp.min(cats, axis=1, keepdims=True)
    high = jnp.max(cats, axis=1, keepdims=True)
    row = jnp.zeros((users, LANES), jnp.float32)
    for step in range(QCAT // 2):
        for place, value in ((step, low), (QCAT - 1 - step, high)):
            row = jnp.where(lane % half == place * users + user, value, row)
        if step + 1 < QCAT // 2:
            above = jnp.min(jnp.where(cats > low, cats, beyond), axis=1, keepdims=True)
            below = jnp.max(jnp.where(cats < high, cats, -beyond), axis=1, keepdims=True)
            low = jnp.where(above == beyond, low, above)
            high = jnp.where(below == -beyond, high, below)
    whole = jnp.sum(row, axis=0, keepdims=True).astype(jnp.int32)
    fine = whole & (FINE - 1)
    packed = jnp.where(iota((1, LANES), 1) < half, whole - fine, fine)
    out_ref[...] = jnp.broadcast_to(packed.reshape(1, 1, LANES), out_ref.shape)


def pack_kernel(wanted_ref, event_ref, history_ref, out_ref, *, own_users):
    devices = wanted_ref.shape[0]
    blocks_events = history_ref.shape[0]
    width = history_ref.shape[2]
    depth = event_ref.shape[1]
    span = depth // blocks_events
    per_group = span // own_users
    pairs = own_users // 2
    half = LANES // 2
    pad = -(-depth // LANES) * LANES
    wanted = wanted_ref[:, 0, :].astype(jnp.float32).astype(jnp.bfloat16)
    line = iota((LANES, pad), 0) % half
    mate = iota((LANES, pad), 1) % own_users
    events = event_ref[...]
    match = None
    for j in range(QCAT):
        spread = jnp.where(line == j * own_users + mate, 1.0, 0.0).astype(jnp.bfloat16)
        category = jnp.dot(wanted, spread, preferred_element_type=jnp.float32)[:, :depth]
        same = jnp.where(category == events, 1.0, 0.0)
        match = same if match is None else jnp.maximum(match, same)
    position = iota((devices, depth), 1) % span
    before = iota((depth, pad), 0)
    here = iota((depth, pad), 1)
    user_before = before % span
    user_here = here % span
    counted = (user_before == user_here) & (before <= here)
    counted = counted | ((user_here % 2 == 1) & (user_before == user_here - 1))
    counted = jnp.where(counted, 1.0, 0.0).astype(jnp.bfloat16)
    matched = match.astype(jnp.bfloat16)
    place = jnp.dot(matched, counted, preferred_element_type=jnp.float32)[:, :depth]
    pair_base = ((position % own_users) // 2 * CAP - 1).astype(jnp.float32)
    code = jnp.where(match > 0.0, place + pair_base, -1.0)
    lane = iota((depth, LANES), 1)
    leading = (lane < pairs) & (iota((depth, LANES), 0) % own_users == 2 * lane)
    leading = jnp.where(leading, 1.0, 0.0).astype(jnp.bfloat16)
    lead = jnp.dot(matched, leading, preferred_element_type=jnp.float32)
    rows = pairs * CAP
    row = iota((rows, depth), 0).astype(jnp.float32)
    for group in range(devices // per_group):
        stored = history_ref[:, group * span : (group + 1) * span, :].reshape(depth, width)
        picks = []
        for member in range(per_group):
            device = group * per_group + member
            picks.append(jnp.where(row == code[device : device + 1, :], 1.0, 0.0).astype(jnp.bfloat16))
        packed = jnp.dot(jnp.concatenate(picks, axis=0), stored, preferred_element_type=jnp.float32)
        for member in range(per_group):
            device = group * per_group + member
            block = packed[member * rows : (member + 1) * rows, :].astype(jnp.bfloat16)
            out_ref[device, : rows // TILE] = block.reshape(rows // TILE, TILE, width)
            out_ref[device, rows // TILE] = jnp.broadcast_to(lead[device : device + 1, :], (TILE, LANES)).astype(
                jnp.bfloat16
            )


def stage_kernel(
    history_ref, cand_ref, event_ref, stored_ref, query_ref, grouped_ref, cand_scratch, event_scratch, sems, *, own_users
):
    event_copy = pltpu.make_async_copy(event_ref, event_scratch, sems.at[0])
    cand_copy = pltpu.make_async_copy(cand_ref, cand_scratch, sems.at[1])
    events = history_ref.shape[0]
    cuts = [events * part // STREAMS for part in range(STREAMS + 1)]
    history_copies = [
        pltpu.make_async_copy(
            history_ref.at[pl.ds(low, high - low)], stored_ref.at[pl.ds(low, high - low)], sems.at[2 + part]
        )
        for part, (low, high) in enumerate(zip(cuts, cuts[1:]))
    ]
    event_copy.start()
    cand_copy.start()
    for copy in history_copies:
        copy.start()

    event_copy.wait()
    users = event_ref.shape[1]
    devices = users // own_users
    depth = grouped_ref.shape[1]
    span = depth // events
    fold = LANES // span
    owner = iota((devices, users), 1) // own_users == iota((devices, users), 0)
    parts = ([], [])
    for event in range(events):
        line = event_scratch[event : event + 1, :]
        fine = line & (FINE - 1)
        for part, value in zip(parts, (line - fine, fine)):
            part.append(jnp.where(owner, value.astype(jnp.float32), 0.0).astype(jnp.bfloat16))
    spread = jnp.where(iota((users, LANES), 0) % span == iota((users, LANES), 1) % span, 1.0, 0.0).astype(jnp.bfloat16)
    picked = sum(
        jnp.dot(jnp.concatenate(part, axis=0), spread, preferred_element_type=jnp.float32) for part in parts
    )
    lane = iota((devices, LANES), 1)
    mine = lane % span // own_users == iota((devices, LANES), 0) % (span // own_users)
    for first in range(0, events, fold):
        tile = jnp.full((devices, LANES), -1.0, jnp.float32)
        for event in range(first, min(first + fold, events)):
            rows = picked[event * devices : (event + 1) * devices, :]
            tile = jnp.where(mine & (lane // span == event - first), rows, tile)
        low = first * span
        high = min(low + LANES, depth)
        grouped_ref[:, low:high] = tile[:, : high - low]

    cand_copy.wait()
    width = cand_ref.shape[1]
    cand_count = query_ref.shape[1] // HEADS
    head_of = iota((cand_count, width), 1) // (width // HEADS)
    for pair in range(query_ref.shape[0]):
        for member in range(2):
            start = (2 * pair + member) * cand_count
            cands = cand_scratch[start : start + cand_count, :].astype(jnp.float32)
            heads = [jnp.where(head_of == head, cands, 0.0) for head in HEAD_ORDER]
            query_ref[pair, :, member * width : (member + 1) * width] = jnp.concatenate(heads, axis=0).astype(
                jnp.bfloat16
            )
    for copy in history_copies:
        copy.wait()


def chunks(total, most):
    best = total
    for size in range(8, most + 1, 8):
        if total % size == 0 and (size % 16 == 0 or total % 16):
            best = size
    return [(start, best) for start in range(0, total, best)]


def tower_kernel(
    packed_ref, query_ref, cand_ref, w_in_ref, w_out_ref, out_ref,
    score_ref, weight_ref, sum_ref, interest_ref, hidden_ref, active_ref, half_ref, result_ref, sems,
):
    pairs, head_rows, _ = query_ref.shape
    cand_count = head_rows // HEADS
    rows = 2 * cand_count
    width = cand_ref.shape[1]
    devices = packed_ref.shape[0]
    slots = devices * CAP
    head_size = width // HEADS
    scale = math.log2(math.e) * head_size ** (-0.5)
    lead = packed_ref[:, pairs * CAP // TILE].astype(jnp.float32)[:, :1, :]
    rank = iota((devices, CAP, LANES), 1).astype(jnp.float32)
    marks = jnp.where(rank < jnp.broadcast_to(lead, (devices, CAP, LANES)), 1.0, 0.0).reshape(slots, LANES)
    pick = jnp.where(iota((2 * CAP, LANES), 0) == iota((2 * CAP, LANES), 1), 1.0, 0.0).astype(jnp.bfloat16)
    across = lax.dot_general(
        pick, marks.astype(jnp.bfloat16), (((1,), (1,)), ((), ())), preferred_element_type=jnp.float32
    )
    slot_even = ((iota((slots, width), 1) // head_size) % 2).astype(jnp.float32).astype(jnp.bfloat16) == 0
    values = {}
    half_ref[...] = w_in_ref[...] * 0.5

    def score(pair):
        keys = packed_ref[:, pair * CAP // TILE : (pair + 1) * CAP // TILE]
        keys = keys.astype(jnp.float32).reshape(slots, width).astype(jnp.bfloat16)
        owned = jnp.broadcast_to(marks[:, pair : pair + 1], (slots, width)).astype(jnp.bfloat16)
        shared = 1 - owned
        own_keys = (keys * owned, keys * shared)
        right = jnp.concatenate(own_keys, axis=1)
        both = ((own_keys[0], owned), (own_keys[1], shared))
        values[pair] = (
            jnp.concatenate([jnp.where(slot_even, k, o) for k, o in both], axis=1),
            jnp.concatenate([jnp.where(slot_even, o, k) for k, o in both], axis=1),
        )
        score_ref[pair] = lax.dot_general(
            query_ref[pair], right, (((1,), (1,)), ((), ())), preferred_element_type=jnp.float32
        )

    def weigh(pair):
        mark = across[pair : pair + 1, :]
        firsts = mark.astype(jnp.bfloat16) > 0.5
        bar_first = ((1.0 - mark) * BARRED).astype(jnp.bfloat16)
        bar_second = (mark * BARRED).astype(jnp.bfloat16)
        for start, size in chunks(head_rows, 160):
            scores = score_ref[pair, start : start + size, :]
            rough = scores.astype(jnp.bfloat16)
            peak_first = jnp.max(rough + bar_first, axis=1, keepdims=True)
            peak_second = jnp.max(rough + bar_second, axis=1, keepdims=True)
            peak = jnp.where(firsts, peak_first, peak_second).astype(jnp.float32)
            weight_ref[pair, start : start + size, :] = jnp.exp2((scores - peak) * scale).astype(jnp.bfloat16)

    def gather(pair):
        for parity in range(2):
            span = slice(parity * head_rows // 2, (parity + 1) * head_rows // 2)
            sum_ref[pair, span, :] = jnp.dot(
                weight_ref[pair, span, :], values[pair][parity], preferred_element_type=jnp.float32
            )

    def blend(pair):
        for start, size in chunks(cand_count, 40):
            head_of = iota((size, width), 1) // head_size
            for member in range(2):
                parts = [
                    sum_ref[
                        pair,
                        block * cand_count + start : block * cand_count + start + size,
                        member * width : (member + 1) * width,
                    ]
                    for block in map(HEAD_ORDER.index, range(HEADS))
                ]
                top = parts[0]
                total = parts[HEADS - 1]
                for head in range(1, HEADS):
                    top = jnp.where(head_of == head, parts[head], top)
                    total = jnp.where(head_of == head, parts[head - 1], total)
                inverse = pltpu.roll(1.0 / total, width - head_size, 1)
                interest_ref[pair, member * cand_count + start : member * cand_count + start + size, :] = (
                    top * inverse
                )

    def enter(pair):
        joined = jnp.concatenate(
            [cand_ref[pair * rows : (pair + 1) * rows, :], interest_ref[pair].astype(jnp.bfloat16)], axis=1
        )
        hidden_ref[pair] = jnp.dot(joined, half_ref[...], preferred_element_type=jnp.float32)

    def activate(pair):
        for start, size in chunks(rows, 16):
            middle = hidden_ref[pair, start : start + size, :]
            active_ref[pair, start : start + size, :] = (middle * jnp.tanh(middle) + middle).astype(jnp.bfloat16)

    def leave(pair):
        for part, (low, high) in enumerate(halves):
            result = jnp.dot(active_ref[pair, low:high, :], w_out_ref[...], preferred_element_type=jnp.float32)
            result_ref[pair * rows + low : pair * rows + high, :] = result.astype(jnp.bfloat16)
            copy_out(pair, part).start()

    cut = -(-rows // 32) * 16
    halves = ((0, cut), (cut, rows))

    def copy_out(pair, part):
        low, high = halves[part]
        span = pl.ds(pair * rows + low, high - low)
        return pltpu.make_async_copy(result_ref.at[span], out_ref.at[span], sems.at[2 * pair + part])

    stages = (score, weigh, gather, blend, enter, activate, leave)
    begins = [pair // 2 * 5 + (pair % 2 if pair > 1 else 0) for pair in range(pairs)]
    for tick in range(len(stages) + begins[-1]):
        for pair in range(pairs):
            stage = tick - begins[pair]
            if 0 <= stage < len(stages):
                stages[stage](pair)
    for pair in range(pairs):
        for part in range(2):
            copy_out(pair, part).wait()


def near(value):
    return pltpu.with_memory_space_constraint(value, pltpu.VMEM)


def exchange(parts):
    return lax.all_to_all(parts, AXES, split_axis=0, concat_axis=0, tiled=True)


def local(history, event_cat, candidates, cand_cat, w_input, w_output):
    devices = lax.axis_size(AXES)
    own_users, cand_count, width = candidates.shape
    users, block_events = event_cat.shape
    pairs = own_users // 2
    resident = pl.BlockSpec(memory_space=pltpu.VMEM)
    wanted = pl.pallas_call(
        distinct_kernel,
        out_shape=pltpu.VMEM((devices, 1, LANES), jnp.int32),
        out_specs=resident,
        compiler_params=pltpu.CompilerParams(vmem_limit_bytes=4 * MEBI),
        name="distinct",
    )(cand_cat)
    wanted = exchange(wanted)
    by_event = history.transpose(1, 0, 2)
    rows = own_users * cand_count
    flat_cands = candidates.reshape(rows, width)
    span = math.lcm(16, own_users)
    far = pl.BlockSpec(memory_space=pltpu.HBM)
    stored, query, grouped = pl.pallas_call(
        lambda *refs: stage_kernel(*refs, own_users=own_users),
        out_shape=[
            pltpu.VMEM(by_event.shape, jnp.bfloat16),
            pltpu.VMEM((pairs, HEADS * cand_count, 2 * width), jnp.bfloat16),
            pltpu.VMEM((devices, block_events * span), jnp.float32),
        ],
        in_specs=[far] * 3,
        out_specs=[resident] * 3,
        scratch_shapes=[
            pltpu.VMEM((rows, width), jnp.bfloat16),
            pltpu.VMEM((block_events, users), jnp.int32),
            pltpu.SemaphoreType.DMA((2 + STREAMS,)),
        ],
        compiler_params=pltpu.CompilerParams(vmem_limit_bytes=24 * MEBI),
        name="stage",
    )(*[pltpu.with_memory_space_constraint(value, pltpu.HBM) for value in (by_event, flat_cands, event_cat.T)])
    packed = pl.pallas_call(
        lambda *refs: pack_kernel(*refs, own_users=own_users),
        out_shape=pltpu.VMEM((devices, pairs * CAP // TILE + 1, TILE, width), jnp.bfloat16),
        out_specs=resident,
        in_specs=[resident] * 3,
        compiler_params=pltpu.CompilerParams(vmem_limit_bytes=24 * MEBI),
        name="pack",
    )(near(wanted), near(grouped), near(stored))
    received = exchange(packed)
    slots = devices * CAP
    result = pl.pallas_call(
        tower_kernel,
        out_shape=jax.ShapeDtypeStruct((rows, width), jnp.bfloat16),
        in_specs=[resident] * 5,
        out_specs=pl.BlockSpec(memory_space=pltpu.HBM),
        scratch_shapes=[
            pltpu.VMEM((pairs, HEADS * cand_count, slots), jnp.float32),
            pltpu.VMEM((pairs, HEADS * cand_count, slots), jnp.bfloat16),
            pltpu.VMEM((pairs, HEADS * cand_count, 2 * width), jnp.float32),
            pltpu.VMEM((pairs, 2 * cand_count, width), jnp.float32),
            pltpu.VMEM((pairs, 2 * cand_count, w_input.shape[1]), jnp.float32),
            pltpu.VMEM((pairs, 2 * cand_count, w_input.shape[1]), jnp.bfloat16),
            pltpu.VMEM(w_input.shape, jnp.bfloat16),
            pltpu.VMEM((rows, width), jnp.bfloat16),
            pltpu.SemaphoreType.DMA((2 * pairs,)),
        ],
        compiler_params=pltpu.CompilerParams(vmem_limit_bytes=40 * MEBI),
        name="tower",
    )(near(received), near(query), near(flat_cands), near(w_input), near(w_output))
    return result.reshape(own_users, cand_count, width)


def solution(mesh):
    placed = (
        P(None, AXES, None),
        P(None, AXES),
        P(AXES, None, None),
        P(AXES, None),
        P(),
        P(),
    )
    return jax.shard_map(
        local,
        mesh=mesh,
        in_specs=placed,
        out_specs=P(AXES, None, None),
        check_vma=False,
    )
```
